64 devices in a mesh: sys: 4 (over x, y), blk: 16 (over z, core).
Axes of the slice: x: 2, y: 2, z: 8, core: 2. Of those that a mesh axis runs over, the one named last changes fastest.
The devices are a block of a 4x4x8 slice.
Arguments:
- positions: float32 [65536, 256], P(('sys', 'blk')), parts along dimension 0
- velocity: float32 [65536, 256], P(('sys', 'blk')), parts along dimension 0
- charges: float32 [65536], P(('sys', 'blk')), parts along dimension 0
Outputs:
- output 1: float32 [65536, 256], P(('sys', 'blk')), parts along dimension 0
- output 2: float32 [4], P('sys'), parts along dimension 0
- output 3: float32 [65536, 256], P(('sys', 'blk')), parts along dimension 0
- output 4: float32 [65536, 256], P(('sys', 'blk')), parts along dimension 0
There are 4 independent parts. The reference program is written for one: setup_inputs(seed, part) draws one part's arguments, and reference() takes and returns one part's arrays. A program takes and returns all parts, laid end to end along the dimension named above; each array names one.
All inputs are finite; a program needn't handle non-finite values.
Results may differ from the reference program's by a relative error of at most 0.00277111.
Values are sent between devices in bfloat16 or wider.
A program may use at most 768 MiB of HBM per device.

```python
import jax
import jax.numpy as jnp
from jax import lax

GROUP_SIZE = 16
ROWS = 1024
D = 256

N_PART = GROUP_SIZE * ROWS
ROW_TILE = 256
STEP_SIZE = 0.5
ELL_SQ = 1.0 * D
CHARGE_SCALE = (2.0 * D) ** 0.5 * N_PART ** -0.25


def setup_inputs(seed: int = 0, part: int = 0) -> dict:
    key = jax.random.fold_in(jax.random.key(seed), part)
    key_pos, key_spread, key_sign, key_mag, key_vel = jax.random.split(key, 5)
    spread = jax.random.uniform(key_spread, (N_PART, 1), jnp.float32, 0.5, 1.5)
    positions = jax.random.normal(key_pos, (N_PART, D), jnp.float32) * spread
    signs = (2 * jax.random.randint(key_sign, (N_PART,), 0, 2) - 1).astype(jnp.float32)
    charges = signs * jax.random.uniform(key_mag, (N_PART,), jnp.float32, 0.5, 1.5) * CHARGE_SCALE
    velocity = jax.random.normal(key_vel, (N_PART, D), jnp.float32)
    return {"positions": positions, "velocity": velocity, "charges": charges}


def kernel_forces(positions, charges):
    low = positions.astype(jnp.bfloat16)
    sq_norm = jnp.sum(jnp.square(low.astype(jnp.float32)), axis=1)
    col_ids = jnp.arange(N_PART)

    def tile_terms(tile_idx):
        row_start = tile_idx * ROW_TILE
        x_tile = lax.dynamic_slice_in_dim(low, row_start, ROW_TILE, 0)
        q_tile = lax.dynamic_slice_in_dim(charges, row_start, ROW_TILE, 0)
        sq_tile = lax.dynamic_slice_in_dim(sq_norm, row_start, ROW_TILE, 0)
        gram_tile = jnp.dot(x_tile, low.T, preferred_element_type=jnp.float32)
        dist_sq = jnp.maximum(sq_tile[:, None] + sq_norm[None, :] - 2.0 * gram_tile, 0.0)
        weight = q_tile[:, None] * charges[None, :] * jnp.exp(-dist_sq / (2.0 * ELL_SQ))
        on_diag = (row_start + jnp.arange(ROW_TILE))[:, None] == col_ids[None, :]
        weight = jnp.where(on_diag, 0.0, weight)
        pull_sum = jnp.dot(weight.astype(jnp.bfloat16), low, preferred_element_type=jnp.float32)
        force_tile = (jnp.sum(weight, axis=1)[:, None] * x_tile.astype(jnp.float32) - pull_sum) / ELL_SQ
        return force_tile, 0.5 * jnp.sum(weight)

    force_tiles, energy_tiles = lax.map(tile_terms, jnp.arange(N_PART // ROW_TILE))
    return force_tiles.reshape(N_PART, D), jnp.sum(energy_tiles)


def reference(positions, velocity, charges):
    force_zero, _ = kernel_forces(positions, charges)
    pos_one = positions + STEP_SIZE * velocity
    vel_one = velocity + STEP_SIZE * force_zero
    force_one, energy_one = kernel_forces(pos_one, charges)
    pos_two = pos_one + STEP_SIZE * vel_one
    vel_two = vel_one + STEP_SIZE * force_one
    return (force_one, energy_one.reshape(1), pos_two, vel_two)
```

```python
import functools

import jax
import jax.numpy as jnp
from jax import lax
from jax.experimental import pallas as pl
from jax.experimental.pallas import tpu as pltpu
from jax.sharding import PartitionSpec as P

MESH = pl.DeviceIdType.MESH
STEP_SIZE = 0.5
LOG2E = 1.4426950408889634
LANES = 128
F32 = jnp.float32
BF16 = jnp.bfloat16


def kernel(n, x0_ref, v0_ref, q_ref, f1_ref, x2_ref, v2_ref, e_ref,
           xg, xl, aux, sc, qc, acc, rho, ebuf,
           send_r, recv_r, send_l, recv_l, send_s, recv_s, own_send, own_recv,
           asend_r, arecv_r, asend_l, arecv_l, asend_s, arecv_s, esend, erecv):
    rows, dim = x0_ref.shape
    unit = rows // 2
    sub = rows // 4
    chunks = rows // LANES
    half_way = n // 4
    scale = LOG2E / (2.0 * dim)
    me = lax.axis_index("blk")
    right = lax.rem(me + 2, n)
    left = lax.rem(me + n - 2, n)
    sib = me + 1 - 2 * lax.rem(me, 2)

    def push(ref, send, recv, target):
        pltpu.make_async_remote_copy(src_ref=ref, dst_ref=ref, send_sem=send, recv_sem=recv,
                                     device_id={"blk": target}, device_id_type=MESH).start()

    def await_recv(ref, send, recv):
        pltpu.make_async_remote_copy(src_ref=ref, dst_ref=ref, send_sem=send, recv_sem=recv,
                                     device_id={"blk": sib}, device_id_type=MESH).wait_recv()

    def await_send(ref, send, recv):
        pltpu.make_async_remote_copy(src_ref=ref, dst_ref=ref, send_sem=send, recv_sem=recv,
                                     device_id={"blk": sib}, device_id_type=MESH).wait_send()

    def unit_ref(ev, src, half):
        return xg.at[ev, src, pl.ds(pl.multiple_of(half * unit, unit), unit), :]

    barrier = pltpu.get_barrier_semaphore()

    @pl.loop(1, n)
    def _(p):
        pl.semaphore_signal(barrier, inc=1, device_id={"blk": lax.rem(me + p, n)}, device_id_type=MESH)

    aux[me, 0] = q_ref[...]

    @pl.loop(0, chunks)
    def _(c):
        rs = pl.ds(pl.multiple_of(c * LANES, LANES), LANES)
        pos = x0_ref[rs, :]
        for ev in (0, 1):
            if ev == 1:
                pos = pos + STEP_SIZE * v0_ref[rs, :]
            low = pos.astype(BF16)
            xg[ev, me, rs, :] = low
            wide = low.astype(F32)
            xl[ev, rs, :] = (wide * 2.0).astype(BF16)
            norm = jnp.broadcast_to(jnp.sum(wide * wide, axis=1, keepdims=True), (LANES, LANES))
            sc[ev, rs, :] = norm
            aux[me, 1 + ev, pl.ds(c, 1), :] = norm.T[0:1, :]
        qc[rs, :] = jnp.broadcast_to(q_ref[pl.ds(c, 1), :], (LANES, LANES)).T

    acc[...] = jnp.zeros_like(acc)
    rho[...] = jnp.zeros_like(rho)
    pl.semaphore_wait(barrier, n - 1)

    push(aux.at[me], asend_r.at[1], arecv_r.at[1], right)
    push(aux.at[me], asend_l.at[1], arecv_l.at[1], left)
    push(aux.at[me], asend_s.at[0, 0], arecv_s.at[0, 0], sib)
    for v in (1, 2, 3, 4):
        ev, hr = 1 - (v - 1) // 2, (v - 1) % 2
        push(unit_ref(ev, me, hr), send_r.at[v], recv_r.at[v], right)
        push(unit_ref(ev, me, 1 - hr), send_l.at[v], recv_l.at[v], left)
        if v % 2 == 1:
            push(xg.at[ev, me], own_send.at[ev], own_recv.at[ev], sib)

    def pair_unit(ev, src, half, own):
        xj = xg[ev, src, pl.ds(pl.multiple_of(half * unit, unit), unit), :]
        base = half * (unit // LANES)
        if own:
            diff = lax.broadcasted_iota(jnp.int32, (sub, LANES), 0) - lax.broadcasted_iota(jnp.int32, (sub, LANES), 1)
        for r in range(rows // sub):
            rs = pl.ds(r * sub, sub)
            gram = lax.dot_general(xl[ev, rs, :], xj, (((1,), (1,)), ((), ())), preferred_element_type=F32)
            norm_i = sc[ev, rs, :]
            q_i = qc[rs, :]
            low, total = [], None
            for c in range(unit // LANES):
                norm_j = aux[src, 1 + ev, pl.ds(base + c, 1), :]
                q_j = aux[src, 0, pl.ds(base + c, 1), :]
                neg = jnp.minimum(gram[:, c * LANES:(c + 1) * LANES] - (norm_i + norm_j), 0.0)
                weight = (q_i * q_j) * jnp.exp2(neg * scale)
                if own:
                    weight = jnp.where(diff == half * unit + (c * LANES - r * sub), 0.0, weight)
                total = weight if total is None else total + weight
                low.append(weight.astype(BF16))
            rho[ev, rs, :] += total
            acc[ev, rs, :] += jnp.dot(jnp.concatenate(low, axis=1), xj, preferred_element_type=F32)

    def pair_two(ev, src_a, half_a, src_b, half_b):
        @pl.loop(0, 2)
        def _(j):
            pair_unit(ev, src_a + j * (src_b - src_a), half_a + j * (half_b - half_a), False)

    @pl.loop(0, 4)
    def _(j):
        pair_unit(1 - j // 2, me, lax.rem(j, 2), True)

    await_recv(aux.at[sib], asend_s.at[0, 0], arecv_s.at[0, 0])

    @pl.loop(0, 2)
    def _(j):
        await_recv(xg.at[1 - j, sib], own_send.at[1 - j], own_recv.at[1 - j])
        pair_two(1 - j, sib, 0, sib, 1)

    last = 3 * half_way + 2

    @pl.loop(1, last + 1)
    def _(i):
        v = i + i // last
        hop = 1 + (v - 1) // 4
        m = lax.rem(v - 1, 4)
        ev = 1 - m // 2
        hr = lax.rem(m, 2)
        hl = 1 - hr
        src_r = lax.rem(me + n - 2 * hop, n)
        src_l = lax.rem(me + 2 * hop, n)
        sib_r = lax.rem(sib + n - 2 * hop, n)
        sib_l = lax.rem(sib + 2 * hop, n)
        onward = (hop < half_way - 1) | ((hop < half_way) & (hr == 0))

        @pl.when(m == 0)
        def _():
            await_recv(aux.at[src_r], asend_r.at[hop], arecv_r.at[hop])
            push(aux.at[src_r], asend_s.at[0, hop], arecv_s.at[0, hop], sib)

            @pl.when(hop < half_way)
            def _():
                push(aux.at[src_r], asend_r.at[hop + 1], arecv_r.at[hop + 1], right)
                await_recv(aux.at[src_l], asend_l.at[hop], arecv_l.at[hop])
                push(aux.at[src_l], asend_s.at[1, hop], arecv_s.at[1, hop], sib)

                @pl.when(hop < half_way - 1)
                def _():
                    push(aux.at[src_l], asend_l.at[hop + 1], arecv_l.at[hop + 1], left)

        await_recv(unit_ref(ev, src_r, hr), send_r.at[v], recv_r.at[v])

        @pl.when(onward)
        def _():
            push(unit_ref(ev, src_r, hr), send_r.at[v + 4], recv_r.at[v + 4], right)

        push(unit_ref(ev, src_r, hr), send_s.at[0, v], recv_s.at[0, v], sib)
        await_recv(unit_ref(ev, src_l, hl), send_l.at[v], recv_l.at[v])

        @pl.when(onward)
        def _():
            push(unit_ref(ev, src_l, hl), send_l.at[v + 4], recv_l.at[v + 4], left)

        push(unit_ref(ev, src_l, hl), send_s.at[1, v], recv_s.at[1, v], sib)

        @pl.when(i == last)
        def _():
            @pl.loop(1, n)
            def _(p):
                peer = lax.rem(me + p, n)
                push(ebuf.at[me], esend.at[peer], erecv.at[me], peer)

        pair_two(ev, src_r, hr, src_l, hl)

        @pl.when(m == 0)
        def _():
            await_recv(aux.at[sib_r], asend_s.at[0, hop], arecv_s.at[0, hop])

            @pl.when(hop < half_way)
            def _():
                await_recv(aux.at[sib_l], asend_s.at[1, hop], arecv_s.at[1, hop])

        await_recv(unit_ref(ev, sib_r, hr), send_s.at[0, v], recv_s.at[0, v])
        await_recv(unit_ref(ev, sib_l, hl), send_s.at[1, v], recv_s.at[1, v])
        pair_two(ev, sib_r, hr, sib_l, hl)

        @pl.when(i == last - 1)
        def _():
            ebuf[me] = jnp.broadcast_to(0.5 * jnp.sum(rho[1], keepdims=True), ebuf.shape[1:])

    @pl.loop(0, chunks)
    def _(c):
        rs = pl.ds(pl.multiple_of(c * LANES, LANES), LANES)
        force = [(jnp.sum(rho[ev, rs, :], axis=1, keepdims=True) * xg[ev, me, rs, :].astype(F32) - acc[ev, rs, :])
                 / dim for ev in (0, 1)]
        vel_zero = v0_ref[rs, :]
        vel_one = vel_zero + STEP_SIZE * force[0]
        f1_ref[rs, :] = force[1]
        x2_ref[rs, :] = (x0_ref[rs, :] + STEP_SIZE * vel_zero) + STEP_SIZE * vel_one
        v2_ref[rs, :] = vel_one + STEP_SIZE * force[1]

    @pl.loop(1, n)
    def _(p):
        peer = lax.rem(me + p, n)
        await_recv(ebuf.at[peer], esend.at[peer], erecv.at[peer])
        await_send(ebuf.at[me], esend.at[peer], erecv.at[me])

    e_ref[0] = jnp.sum(jnp.sum(ebuf[...], axis=0)[0:1, 0:1])

    @pl.loop(1, last + 1)
    def _(i):
        v = i + i // last
        piece = unit_ref(0, me, 0)
        await_send(piece, send_r.at[v], recv_r.at[v])
        await_send(piece, send_l.at[v], recv_l.at[v])
        await_send(piece, send_s.at[0, v], recv_s.at[0, v])
        await_send(piece, send_s.at[1, v], recv_s.at[1, v])

    for ev in (0, 1):
        await_send(xg.at[ev, me], own_send.at[ev], own_recv.at[ev])
    table = aux.at[me]
    await_send(table, asend_s.at[0, 0], arecv_s.at[0, 0])
    for hop in range(1, half_way + 1):
        await_send(table, asend_r.at[hop], arecv_r.at[hop])
        await_send(table, asend_s.at[0, hop], arecv_s.at[0, hop])
        if hop < half_way:
            await_send(table, asend_l.at[hop], arecv_l.at[hop])
            await_send(table, asend_s.at[1, hop], arecv_s.at[1, hop])


def solution(mesh):
    n = mesh.shape["blk"]
    row_spec = P(("sys", "blk"), None)
    vec_spec = P(("sys", "blk"))

    def local_steps(positions, velocity, charges):
        rows, dim = positions.shape
        hops = n // 4
        pieces = 4 * hops + 1
        dma = pltpu.SemaphoreType.DMA
        whole = pl.BlockSpec(memory_space=pltpu.VMEM)
        flat = jax.ShapeDtypeStruct((rows, dim), F32)
        force_one, pos_two, vel_two, energy = pl.pallas_call(
            functools.partial(kernel, n),
            out_shape=(flat, flat, flat, jax.ShapeDtypeStruct((1,), F32)),
            in_specs=[whole] * 3,
            out_specs=(whole, whole, whole, pl.BlockSpec(memory_space=pltpu.SMEM)),
            scratch_shapes=[
                pltpu.VMEM((2, n, rows, dim), BF16),
                pltpu.VMEM((2, rows, dim), BF16),
                pltpu.VMEM((n, 3, rows // LANES, LANES), F32),
                pltpu.VMEM((2, rows, LANES), F32),
                pltpu.VMEM((rows, LANES), F32),
                pltpu.VMEM((2, rows, dim), F32),
                pltpu.VMEM((2, rows, LANES), F32),
                pltpu.VMEM((n, 8, LANES), F32),
                dma((pieces,)), dma((pieces,)), dma((pieces,)), dma((pieces,)),
                dma((2, pieces)), dma((2, pieces)), dma((2,)), dma((2,)),
                dma((hops + 1,)), dma((hops + 1,)), dma((hops + 1,)), dma((hops + 1,)),
                dma((2, hops + 1)), dma((2, hops + 1)), dma((n,)), dma((n,)),
            ],
            compiler_params=pltpu.CompilerParams(collective_id=0, has_side_effects=True, vmem_limit_bytes=56 << 20),
            name="leapfrog",
        )(positions, velocity, charges.reshape(rows // LANES, LANES))
        return force_one, energy, pos_two, vel_two

    return jax.shard_map(local_steps, mesh=mesh, in_specs=(row_spec, row_spec, vec_spec),
                         out_specs=(row_spec, P("sys"), row_spec, row_spec), check_vma=False)
```

```python
import functools

import jax
import jax.numpy as jnp
from jax import lax
from jax.experimental import pallas as pl
from jax.experimental.pallas import tpu as pltpu
from jax.sharding import PartitionSpec as P

MESH = pl.DeviceIdType.MESH
STEP_SIZE = 0.5
LOG2E = 1.4426950408889634
LANES = 128
F32 = jnp.float32
BF16 = jnp.bfloat16


def kernel(n, x0_hbm, v0_hbm, q_hbm, f0_ref, f1_ref, e_ref,
           x0_ref, v0_ref, xg, xl, aux, sc, qc, acc, rho, ebuf, in_sem,
           send_r, recv_r, send_l, recv_l, send_s, recv_s, own_send, own_recv,
           asend_r, arecv_r, asend_l, arecv_l, asend_s, arecv_s, esend, erecv):
    rows, dim = x0_ref.shape
    unit = rows // 2
    sub = rows // 4
    chunks = rows // LANES
    half_way = n // 4
    scale = LOG2E / (2.0 * dim)
    me = lax.axis_index("blk")
    right = lax.rem(me + 2, n)
    left = lax.rem(me + n - 2, n)
    sib = me + 1 - 2 * lax.rem(me, 2)

    def push(ref, send, recv, target):
        pltpu.make_async_remote_copy(src_ref=ref, dst_ref=ref, send_sem=send, recv_sem=recv,
                                     device_id={"blk": target}, device_id_type=MESH).start()

    def await_recv(ref, send, recv):
        pltpu.make_async_remote_copy(src_ref=ref, dst_ref=ref, send_sem=send, recv_sem=recv,
                                     device_id={"blk": sib}, device_id_type=MESH).wait_recv()

    def await_send(ref, send, recv):
        pltpu.make_async_remote_copy(src_ref=ref, dst_ref=ref, send_sem=send, recv_sem=recv,
                                     device_id={"blk": sib}, device_id_type=MESH).wait_send()

    def unit_ref(ev, src, half):
        return xg.at[ev, src, pl.ds(pl.multiple_of(half * unit, unit), unit), :]

    barrier = pltpu.get_barrier_semaphore()
    for peer in (left, right, sib):
        pl.semaphore_signal(barrier, inc=1, device_id={"blk": peer}, device_id_type=MESH)
    loads = [pltpu.make_async_copy(src, dst, in_sem.at[k])
             for k, (src, dst) in enumerate(((q_hbm, aux.at[me, 0]), (v0_hbm, v0_ref), (x0_hbm, x0_ref)))]
    for load in loads:
        load.start()

    loads[0].wait()
    for c in range(chunks):
        qc[c * LANES:(c + 1) * LANES, :] = jnp.broadcast_to(aux[me, 0, c:c + 1, :], (LANES, LANES)).T
    for load in loads[1:]:
        load.wait()

    @pl.loop(0, chunks)
    def _(c):
        rs = pl.ds(pl.multiple_of(c * LANES, LANES), LANES)
        xg[1, me, rs, :] = (x0_ref[rs, :] + STEP_SIZE * v0_ref[rs, :]).astype(BF16)

    @pl.loop(0, chunks)
    def _(c):
        rs = pl.ds(pl.multiple_of(c * LANES, LANES), LANES)
        xg[0, me, rs, :] = x0_ref[rs, :].astype(BF16)

    pl.semaphore_wait(barrier, 3)

    def push_own(v):
        ev, hr = 1 - (v - 1) // 2, (v - 1) % 2
        push(unit_ref(ev, me, hr), send_r.at[v], recv_r.at[v], right)
        push(unit_ref(ev, me, 1 - hr), send_l.at[v], recv_l.at[v], left)

    push_own(1)
    push_own(2)
    push(xg.at[1, me], own_send.at[1], own_recv.at[1], sib)

    @pl.loop(0, chunks)
    def _(c):
        rs = pl.ds(pl.multiple_of(c * LANES, LANES), LANES)
        for ev in (1, 0):
            wide = xg[ev, me, rs, :].astype(F32)
            xl[ev, rs, :] = (wide * 2.0).astype(BF16)
            norm = jnp.broadcast_to(jnp.sum(wide * wide, axis=1, keepdims=True), (LANES, LANES))
            sc[ev, rs, :] = norm
            aux[me, 1 + ev, pl.ds(c, 1), :] = norm.T[0:1, :]

    acc[...] = jnp.zeros_like(acc)
    rho[...] = jnp.zeros_like(rho)
    push(aux.at[me], asend_s.at[0, 0], arecv_s.at[0, 0], sib)
    push(aux.at[me], asend_r.at[1], arecv_r.at[1], right)
    push(aux.at[me], asend_l.at[1], arecv_l.at[1], left)
    push_own(3)
    push_own(4)
    push(xg.at[0, me], own_send.at[0], own_recv.at[0], sib)

    def pair_unit(ev, src, start, width, own):
        xj = xg[ev, src, pl.ds(pl.multiple_of(start, width), width), :]
        base = start // LANES
        if own:
            diff = lax.broadcasted_iota(jnp.int32, (sub, LANES), 0) - lax.broadcasted_iota(jnp.int32, (sub, LANES), 1)
        for r in range(rows // sub):
            rs = pl.ds(r * sub, sub)
            gram = lax.dot_general(xl[ev, rs, :], xj, (((1,), (1,)), ((), ())), preferred_element_type=F32)
            norm_i = sc[ev, rs, :]
            q_i = qc[rs, :]
            low, total = [], None
            for c in range(width // LANES):
                norm_j = aux[src, 1 + ev, pl.ds(base + c, 1), :]
                q_j = aux[src, 0, pl.ds(base + c, 1), :]
                neg = jnp.minimum(gram[:, c * LANES:(c + 1) * LANES] - (norm_i + norm_j), 0.0)
                weight = (q_i * q_j) * jnp.exp2(neg * scale)
                if own:
                    weight = jnp.where(diff == start + (c * LANES - r * sub), 0.0, weight)
                total = weight if total is None else total + weight
                low.append(weight.astype(BF16))
            rho[ev, rs, :] += total
            acc[ev, rs, :] += jnp.dot(jnp.concatenate(low, axis=1), xj, preferred_element_type=F32)

    def pair_two(ev, src_a, start_a, src_b, start_b, width):
        @pl.loop(0, 2)
        def _(j):
            pair_unit(ev, src_a + j * (src_b - src_a), start_a + j * (start_b - start_a), width, False)

    @pl.loop(0, 4)
    def _(j):
        pair_unit(1 - j // 2, me, lax.rem(j, 2) * unit, unit, True)

    await_recv(aux.at[sib], asend_s.at[0, 0], arecv_s.at[0, 0])

    @pl.loop(0, 2)
    def _(j):
        await_recv(xg.at[1 - j, sib], own_send.at[1 - j], own_recv.at[1 - j])
        pair_two(1 - j, sib, 0, sib, unit, unit)

    full = 4 * (half_way - 1)
    part = unit // 2

    def part_ref(src, half, p):
        return xg.at[0, src, pl.ds(pl.multiple_of(half * unit + p * part, part), part), :]

    @pl.loop(1, full + 2)
    def _(v):
        hop = 1 + (v - 1) // 4
        m = lax.rem(v - 1, 4)
        ev = 1 - m // 2
        hr = lax.rem(m, 2)
        hl = 1 - hr
        src_r = lax.rem(me + n - 2 * hop, n)
        src_l = lax.rem(me + 2 * hop, n)
        sib_r = lax.rem(sib + n - 2 * hop, n)
        sib_l = lax.rem(sib + 2 * hop, n)
        onward = (v <= full - 4) | (v == full - 3)
        parted = v == full - 1

        @pl.when(m == 0)
        def _():
            await_recv(aux.at[src_r], asend_r.at[hop], arecv_r.at[hop])
            push(aux.at[src_r], asend_s.at[0, hop], arecv_s.at[0, hop], sib)

            @pl.when(hop < half_way)
            def _():
                push(aux.at[src_r], asend_r.at[hop + 1], arecv_r.at[hop + 1], right)
                await_recv(aux.at[src_l], asend_l.at[hop], arecv_l.at[hop])
                push(aux.at[src_l], asend_s.at[1, hop], arecv_s.at[1, hop], sib)

                @pl.when(hop < half_way - 1)
                def _():
                    push(aux.at[src_l], asend_l.at[hop + 1], arecv_l.at[hop + 1], left)

        def take(k, src, half, send, recv, target):
            await_recv(unit_ref(ev, src, half), send.at[v], recv.at[v])

            @pl.when(onward)
            def _():
                push(unit_ref(ev, src, half), send.at[v + 4], recv.at[v + 4], target)

            @pl.when(parted)
            def _():
                for p in (0, 1):
                    push(part_ref(src, half, p), send.at[v + 4 + p], recv.at[v + 4 + p], target)

            push(unit_ref(ev, src, half), send_s.at[k, v], recv_s.at[k, v], sib)

        take(0, src_r, hr, send_r, recv_r, right)
        take(1, src_l, hl, send_l, recv_l, left)
        pair_two(ev, src_r, hr * unit, src_l, hl * unit, unit)

        @pl.when(m == 0)
        def _():
            await_recv(aux.at[sib_r], asend_s.at[0, hop], arecv_s.at[0, hop])

            @pl.when(hop < half_way)
            def _():
                await_recv(aux.at[sib_l], asend_s.at[1, hop], arecv_s.at[1, hop])

        await_recv(unit_ref(ev, sib_r, hr), send_s.at[0, v], recv_s.at[0, v])
        await_recv(unit_ref(ev, sib_l, hl), send_s.at[1, v], recv_s.at[1, v])
        pair_two(ev, sib_r, hr * unit, sib_l, hl * unit, unit)

    def force(ev, out_ref):
        @pl.loop(0, chunks)
        def _(c):
            rs = pl.ds(pl.multiple_of(c * LANES, LANES), LANES)
            held = jnp.sum(rho[ev, rs, :], axis=1, keepdims=True)
            out_ref[rs, :] = held * xg[ev, me, rs, :].astype(F32) - acc[ev, rs, :]

    ebuf[me] = jnp.broadcast_to(0.5 * jnp.sum(rho[1], keepdims=True), ebuf.shape[1:])
    force(1, f1_ref)

    far = lax.rem(me + 2 * half_way, n)
    far_sib = lax.rem(sib + 2 * half_way, n)

    @pl.loop(0, 2)
    def _(p):
        v = full + 3 + p
        await_recv(part_ref(far, 0, p), send_r.at[v], recv_r.at[v])
        push(part_ref(far, 0, p), send_s.at[0, v], recv_s.at[0, v], sib)
        await_recv(part_ref(far, 1, p), send_l.at[v], recv_l.at[v])
        push(part_ref(far, 1, p), send_s.at[1, v], recv_s.at[1, v], sib)

        @pl.when(p == 0)
        def _():
            @pl.loop(1, n)
            def _(k):
                peer = lax.rem(me + k, n)
                push(ebuf.at[me], esend.at[peer], erecv.at[me], peer)

        pair_two(0, far, p * part, far, unit + p * part, part)
        await_recv(part_ref(far_sib, 0, p), send_s.at[0, v], recv_s.at[0, v])
        await_recv(part_ref(far_sib, 1, p), send_s.at[1, v], recv_s.at[1, v])
        pair_two(0, far_sib, p * part, far_sib, unit + p * part, part)

    force(0, f0_ref)

    @pl.loop(1, n)
    def _(p):
        peer = lax.rem(me + p, n)
        await_recv(ebuf.at[peer], esend.at[peer], erecv.at[peer])
        await_send(ebuf.at[me], esend.at[peer], erecv.at[me])

    e_ref[0] = jnp.sum(jnp.sum(ebuf[...], axis=0)[0:1, 0:1])

    @pl.loop(1, full + 2)
    def _(v):
        piece = unit_ref(0, me, 0)
        await_send(piece, send_r.at[v], recv_r.at[v])
        await_send(piece, send_l.at[v], recv_l.at[v])
        await_send(piece, send_s.at[0, v], recv_s.at[0, v])
        await_send(piece, send_s.at[1, v], recv_s.at[1, v])

    for v in (full + 3, full + 4):
        piece = part_ref(me, 0, 0)
        await_send(piece, send_r.at[v], recv_r.at[v])
        await_send(piece, send_l.at[v], recv_l.at[v])
        await_send(piece, send_s.at[0, v], recv_s.at[0, v])
        await_send(piece, send_s.at[1, v], recv_s.at[1, v])

    for ev in (0, 1):
        await_send(xg.at[ev, me], own_send.at[ev], own_recv.at[ev])
    table = aux.at[me]
    await_send(table, asend_s.at[0, 0], arecv_s.at[0, 0])
    for hop in range(1, half_way + 1):
        await_send(table, asend_r.at[hop], arecv_r.at[hop])
        await_send(table, asend_s.at[0, hop], arecv_s.at[0, hop])
        if hop < half_way:
            await_send(table, asend_l.at[hop], arecv_l.at[hop])
            await_send(table, asend_s.at[1, hop], arecv_s.at[1, hop])


def solution(mesh):
    n = mesh.shape["blk"]
    row_spec = P(("sys", "blk"), None)
    vec_spec = P(("sys", "blk"))

    def local_steps(positions, velocity, charges):
        rows, dim = positions.shape
        hops = n // 4
        pieces = 4 * hops + 1
        dma = pltpu.SemaphoreType.DMA
        whole = pl.BlockSpec(memory_space=pltpu.VMEM)
        flat = jax.ShapeDtypeStruct((rows, dim), F32)
        force_zero, force_one, energy = pl.pallas_call(
            functools.partial(kernel, n),
            out_shape=(flat, flat, jax.ShapeDtypeStruct((1,), F32)),
            in_specs=[pl.BlockSpec(memory_space=pltpu.HBM)] * 3,
            out_specs=(whole, whole, pl.BlockSpec(memory_space=pltpu.SMEM)),
            scratch_shapes=[
                pltpu.VMEM((rows, dim), F32),
                pltpu.VMEM((rows, dim), F32),
                pltpu.VMEM((2, n, rows, dim), BF16),
                pltpu.VMEM((2, rows, dim), BF16),
                pltpu.VMEM((n, 3, rows // LANES, LANES), F32),
                pltpu.VMEM((2, rows, LANES), F32),
                pltpu.VMEM((rows, LANES), F32),
                pltpu.VMEM((2, rows, dim), F32),
                pltpu.VMEM((2, rows, LANES), F32),
                pltpu.VMEM((n, 8, LANES), F32),
                dma((3,)),
                dma((pieces,)), dma((pieces,)), dma((pieces,)), dma((pieces,)),
                dma((2, pieces)), dma((2, pieces)), dma((2,)), dma((2,)),
                dma((hops + 1,)), dma((hops + 1,)), dma((hops + 1,)), dma((hops + 1,)),
                dma((2, hops + 1)), dma((2, hops + 1)), dma((n,)), dma((n,)),
            ],
            compiler_params=pltpu.CompilerParams(collective_id=0, has_side_effects=True, vmem_limit_bytes=40 << 20),
            name="leapfrog",
        )(*(pltpu.with_memory_space_constraint(a, pltpu.HBM) for a in
             (positions, velocity, charges.reshape(rows // LANES, LANES))))
        force_zero, force_one = force_zero / dim, force_one / dim
        vel_one = velocity + STEP_SIZE * force_zero
        pos_two = (positions + STEP_SIZE * velocity) + STEP_SIZE * vel_one
        return force_one, energy, pos_two, vel_one + STEP_SIZE * force_one

    return jax.shard_map(local_steps, mesh=mesh, in_specs=(row_spec, row_spec, vec_spec),
                         out_specs=(row_spec, P("sys"), row_spec, row_spec), check_vma=False)
```

```python
import functools

import jax
import jax.numpy as jnp
from jax import lax
from jax.experimental import pallas as pl
from jax.experimental.pallas import tpu as pltpu
from jax.sharding import PartitionSpec as P

MESH = pl.DeviceIdType.MESH
STEP_SIZE = 0.5
LOG2E = 1.4426950408889634
LANES = 128
F32 = jnp.float32
BF16 = jnp.bfloat16


def kernel(n, x0_hbm, v0_hbm, q_hbm, f0_ref, f1_ref, e_ref,
           x0_ref, v0_ref, xg, aux, sc, qc, acc, rho, pout, pin, ebuf, in_sem,
           csend, crecv, tsend, trecv, ssend, srecv, own_send, own_recv,
           asend_r, arecv_r, asend_l, arecv_l, asend_s, arecv_s, psend, precv, esend, erecv):
    rows, dim = x0_ref.shape
    unit = rows // 2
    sub = rows // 4
    chunks = rows // LANES
    hops = n // 4 - 1
    scale = 2.0 * LOG2E / (2.0 * dim)
    me = lax.axis_index("blk")
    right = lax.rem(me + 2, n)
    left = lax.rem(me + n - 2, n)
    sib = me + 1 - 2 * lax.rem(me, 2)
    turn = 1 - 2 * lax.rem(me // 2, 2)

    def side(ev):
        return turn * (1 - 2 * ev)

    def away(dev, ev, hop):
        return lax.rem(dev + n - 2 * side(ev) * hop, n)

    def toward(dev, ev, hop):
        return lax.rem(dev + n + 2 * side(ev) * hop, n)

    def push(ref, send, recv, target, dst=None):
        pltpu.make_async_remote_copy(src_ref=ref, dst_ref=ref if dst is None else dst, send_sem=send, recv_sem=recv,
                                     device_id={"blk": target}, device_id_type=MESH).start()

    def await_recv(ref, send, recv):
        pltpu.make_async_remote_copy(src_ref=ref, dst_ref=ref, send_sem=send, recv_sem=recv,
                                     device_id={"blk": sib}, device_id_type=MESH).wait_recv()

    def await_send(ref, send, recv):
        pltpu.make_async_remote_copy(src_ref=ref, dst_ref=ref, send_sem=send, recv_sem=recv,
                                     device_id={"blk": sib}, device_id_type=MESH).wait_send()

    def span(c):
        return pl.ds(pl.multiple_of(c * LANES, LANES), LANES)

    def piece(ev, src, half):
        return xg.at[ev, src, pl.ds(pl.multiple_of(half * unit, unit), unit), :]

    barrier = pltpu.get_barrier_semaphore()
    for peer in (left, right, sib):
        pl.semaphore_signal(barrier, inc=1, device_id={"blk": peer}, device_id_type=MESH)
    loads = [pltpu.make_async_copy(src, dst, in_sem.at[k])
             for k, (src, dst) in enumerate(((q_hbm, aux.at[me, 0]), (v0_hbm, v0_ref), (x0_hbm, x0_ref)))]
    for load in loads:
        load.start()

    loads[0].wait()
    for c in range(chunks):
        qc[0, c * LANES:(c + 1) * LANES, :] = jnp.broadcast_to(aux[me, 0, c:c + 1, :], (LANES, LANES)).T
    for load in loads[1:]:
        load.wait()

    @pl.loop(0, chunks)
    def _(c):
        xg[1, me, span(c), :] = (x0_ref[span(c), :] + STEP_SIZE * v0_ref[span(c), :]).astype(BF16)

    @pl.loop(0, chunks)
    def _(c):
        xg[0, me, span(c), :] = x0_ref[span(c), :].astype(BF16)

    pl.semaphore_wait(barrier, 3)

    def c_push(ev, src, k, half):
        push(piece(ev, src, half), csend.at[ev, k], crecv.at[ev, k], away(me, ev, 1))

    def t_push(ev, src, k, half):
        push(piece(ev, src, half), tsend.at[ev, k], trecv.at[ev, k], toward(me, ev, 1))

    for ev in (1, 0):
        c_push(ev, me, 0, 0)
        push(xg.at[ev, me], own_send.at[ev], own_recv.at[ev], sib)

    @pl.loop(0, chunks)
    def _(c):
        for ev in (1, 0):
            wide = xg[ev, me, span(c), :].astype(F32)
            norm = jnp.broadcast_to(0.5 * jnp.sum(wide * wide, axis=1, keepdims=True), (LANES, LANES))
            sc[ev, 0, span(c), :] = norm
            aux[me, 1 + ev, pl.ds(c, 1), :] = norm.T[0:1, :]

    acc[...] = jnp.zeros_like(acc)
    rho[...] = jnp.zeros_like(rho)
    push(aux.at[me], asend_s.at[0, 0], arecv_s.at[0, 0], sib)
    push(aux.at[me], asend_r.at[1], arecv_r.at[1], right)
    push(aux.at[me], asend_l.at[1], arecv_l.at[1], left)
    for ev in (1, 0):
        c_push(ev, me, 1, 1)
    for half in (0, 1):
        for ev in (1, 0):
            t_push(ev, me, half, half)

    def pair_unit(ev, party, src, half, own=False):
        mine = toward(me, ev, party)
        xj = xg[ev, src, pl.ds(pl.multiple_of(half * unit, unit), unit), :]
        base = half * (unit // LANES)
        charge = party * (1 + ev)
        if own:
            diff = lax.broadcasted_iota(jnp.int32, (sub, LANES), 0) - lax.broadcasted_iota(jnp.int32, (sub, LANES), 1)
        for r in range(rows // sub):
            rs = pl.ds(r * sub, sub)
            gram = lax.dot_general(xg[ev, mine, rs, :], xj, (((1,), (1,)), ((), ())), preferred_element_type=F32)
            norm_i = sc[ev, party, rs, :]
            q_i = qc[charge, rs, :]
            low, total = [], None
            for c in range(unit // LANES):
                norm_j = aux[src, 1 + ev, pl.ds(base + c, 1), :]
                q_j = aux[src, 0, pl.ds(base + c, 1), :]
                neg = jnp.minimum(gram[:, c * LANES:(c + 1) * LANES] - (norm_i + norm_j), 0.0)
                weight = (q_i * q_j) * jnp.exp2(neg * scale)
                if own:
                    weight = jnp.where(diff == half * unit + (c * LANES - r * sub), 0.0, weight)
                total = weight if total is None else total + weight
                low.append(weight.astype(BF16))
            rho[ev, party, rs, :] += total
            acc[ev, party, rs, :] += jnp.dot(jnp.concatenate(low, axis=1), xj, preferred_element_type=F32)

    @pl.loop(0, 4)
    def _(j):
        pair_unit(1 - j // 2, 0, me, lax.rem(j, 2), own=True)

    await_recv(aux.at[sib], asend_s.at[0, 0], arecv_s.at[0, 0])
    for ev in (1, 0):
        await_recv(xg.at[ev, sib], own_send.at[ev], own_recv.at[ev])

    @pl.loop(0, 4)
    def _(j):
        pair_unit(1 - j // 2, 0, sib, lax.rem(j, 2))

    def table_in(hop):
        for k, (step, send, recv, target) in enumerate(((n - 2 * hop, asend_r, arecv_r, right),
                                                        (2 * hop, asend_l, arecv_l, left))):
            src = lax.rem(me + step, n)
            await_recv(aux.at[src], send.at[hop], recv.at[hop])
            push(aux.at[src], asend_s.at[k, hop], arecv_s.at[k, hop], sib)
            if hop < hops:
                push(aux.at[src], send.at[hop + 1], recv.at[hop + 1], target)

    def table_sib(hop):
        for k, step in enumerate((n - 2 * hop, 2 * hop)):
            await_recv(aux.at[lax.rem(sib + step, n)], asend_s.at[k, hop], arecv_s.at[k, hop])

    def c_take(ev, hop, half):
        k = 2 * (hop - 1) + half
        src = away(me, ev, hop)
        await_recv(piece(ev, src, half), csend.at[ev, k], crecv.at[ev, k])
        push(piece(ev, src, half), ssend.at[ev, k], srecv.at[ev, k], sib)

    def c_sib(ev, hop, half):
        k = 2 * (hop - 1) + half
        await_recv(piece(ev, away(sib, ev, hop), half), ssend.at[ev, k], srecv.at[ev, k])

    def t_take(ev, hop, half):
        k = 2 * (hop - 1) + half
        src = toward(me, ev, hop)
        await_recv(piece(ev, src, half), tsend.at[ev, k], trecv.at[ev, k])
        c_push(ev, src, 2 * hop + half, half)

    @pl.loop(0, 2)
    def _(half):
        for ev in (1, 0):
            c_take(ev, 1, half)
            t_push(ev, away(me, ev, 1), 2 + half, half)

        @pl.when(half == 0)
        def _():
            table_in(1)

        @pl.loop(0, 4)
        def _(j):
            @pl.when(j == 2)
            def _():
                for ev in (1, 0):
                    c_sib(ev, 1, half)

                @pl.when(half == 0)
                def _():
                    table_sib(1)

            ev = 1 - lax.rem(j, 2)
            pair_unit(ev, 0, away(me + (j // 2) * (sib - me), ev, 1), half)

    for half in (0, 1):
        for ev in (1, 0):
            t_take(ev, 1, half)
    table_in(2)

    for ev in (1, 0):
        mate = toward(me, ev, 1)

        @pl.loop(0, chunks)
        def _(c):
            sc[ev, 1, span(c), :] = jnp.broadcast_to(aux[mate, 1 + ev, pl.ds(c, 1), :], (LANES, LANES)).T
            qc[1 + ev, span(c), :] = jnp.broadcast_to(aux[mate, 0, pl.ds(c, 1), :], (LANES, LANES)).T

    @pl.loop(0, 16)
    def _(j):
        @pl.when(j == 8)
        def _():
            for ev in (1, 0):
                t_take(ev, 2, 0)

        ev = lax.rem(j, 2)
        half = lax.rem(j // 2, 2)
        who = lax.rem(j // 4, 2)
        pair_unit(ev, 1, away(me + who * (sib - me), ev, j // 8), half)

    for ev in (1, 0):
        t_take(ev, 2, 1)

    last = 2 * hops - 1

    @pl.loop(2, last)
    def _(k):
        hop = 1 + k // 2
        half = lax.rem(k, 2)
        for ev in (1, 0):
            c_take(ev, hop, half)

        @pl.when(k == last - 1)
        def _():
            table_in(3)

        @pl.loop(0, 8)
        def _(j):
            @pl.when(j == 4)
            def _():
                for ev in (1, 0):
                    c_sib(ev, hop, half)

                @pl.when(k == 2)
                def _():
                    table_sib(2)

                @pl.when(k == last - 1)
                def _():
                    table_sib(3)

            ev = 1 - lax.rem(j // 2, 2)
            pair_unit(ev, lax.rem(j, 2), away(me + (j // 4) * (sib - me), ev, hop), half)

    for ev in (1, 0):
        c_take(ev, hops, 1)

    def last_columns(ev, party):
        @pl.loop(0, 2)
        def _(j):
            if party == 1:
                @pl.when(j == 1)
                def _():
                    c_sib(ev, hops, 1)

            pair_unit(ev, party, away(me + j * (sib - me), ev, hops), 1)

    def force(ev, party, c):
        held = jnp.sum(rho[ev, party, span(c), :], axis=1, keepdims=True)
        return held * xg[ev, toward(me, ev, party), span(c), :].astype(F32) - acc[ev, party, span(c), :]

    def part(ref, ev, half):
        return ref.at[ev, pl.ds(half * unit, unit), :]

    def give(ev, half):
        push(part(pout, ev, half), psend.at[ev, half], precv.at[ev, half], toward(me, ev, 1), part(pin, ev, half))

    for ev in (1, 0):
        last_columns(ev, 1)

        @pl.loop(0, chunks)
        def _(c):
            pout[ev, span(c), :] = force(ev, 1, c).astype(BF16)

        give(ev, 0)

    last_columns(1, 0)
    ebuf[me] = jnp.broadcast_to(0.5 * jnp.sum(rho[1, 0] + rho[1, 1], keepdims=True), ebuf.shape[1:])

    @pl.loop(0, chunks)
    def _(c):
        f1_ref[span(c), :] = force(1, 0, c)

    @pl.loop(1, n)
    def _(k):
        peer = lax.rem(me + k, n)
        push(ebuf.at[me], esend.at[peer], erecv.at[me], peer)

    give(1, 1)
    give(0, 1)
    last_columns(0, 0)

    @pl.loop(0, chunks)
    def _(c):
        f0_ref[span(c), :] = force(0, 0, c)

    for half in (0, 1):
        for ev, out_ref in ((1, f1_ref), (0, f0_ref)):
            await_recv(part(pin, ev, half), psend.at[ev, half], precv.at[ev, half])

            @pl.loop(half * (chunks // 2), (half + 1) * (chunks // 2))
            def _(c):
                out_ref[span(c), :] += pin[ev, span(c), :].astype(F32)

    @pl.loop(1, n)
    def _(p):
        peer = lax.rem(me + p, n)
        await_recv(ebuf.at[peer], esend.at[peer], erecv.at[peer])
        await_send(ebuf.at[me], esend.at[peer], erecv.at[me])

    e_ref[0] = jnp.sum(jnp.sum(ebuf[...], axis=0)[0:1, 0:1])

    for ev in (0, 1):
        @pl.loop(0, 2 * hops)
        def _(k):
            await_send(piece(ev, me, 0), csend.at[ev, k], crecv.at[ev, k])
            await_send(piece(ev, me, 0), ssend.at[ev, k], srecv.at[ev, k])

        @pl.loop(0, 2 * hops - 2)
        def _(k):
            await_send(piece(ev, me, 0), tsend.at[ev, k], trecv.at[ev, k])

        await_send(xg.at[ev, me], own_send.at[ev], own_recv.at[ev])
        for half in (0, 1):
            await_send(part(pout, ev, half), psend.at[ev, half], precv.at[ev, half])

    table = aux.at[me]
    await_send(table, asend_s.at[0, 0], arecv_s.at[0, 0])
    for hop in range(1, hops + 1):
        await_send(table, asend_r.at[hop], arecv_r.at[hop])
        await_send(table, asend_l.at[hop], arecv_l.at[hop])
        await_send(table, asend_s.at[0, hop], arecv_s.at[0, hop])
        await_send(table, asend_s.at[1, hop], arecv_s.at[1, hop])


def solution(mesh):
    n = mesh.shape["blk"]
    row_spec = P(("sys", "blk"), None)
    vec_spec = P(("sys", "blk"))

    def local_steps(positions, velocity, charges):
        rows, dim = positions.shape
        hops = n // 4 - 1
        dma = pltpu.SemaphoreType.DMA
        whole = pl.BlockSpec(memory_space=pltpu.VMEM)
        flat = jax.ShapeDtypeStruct((rows, dim), F32)
        force_zero, force_one, energy = pl.pallas_call(
            functools.partial(kernel, n),
            out_shape=(flat, flat, jax.ShapeDtypeStruct((1,), F32)),
            in_specs=[pl.BlockSpec(memory_space=pltpu.HBM)] * 3,
            out_specs=(whole, whole, pl.BlockSpec(memory_space=pltpu.SMEM)),
            scratch_shapes=[
                pltpu.VMEM((rows, dim), F32),
                pltpu.VMEM((rows, dim), F32),
                pltpu.VMEM((2, n, rows, dim), BF16),
                pltpu.VMEM((n, 3, rows // LANES, LANES), F32),
                pltpu.VMEM((2, 2, rows, LANES), F32),
                pltpu.VMEM((3, rows, LANES), F32),
                pltpu.VMEM((2, 2, rows, dim), F32),
                pltpu.VMEM((2, 2, rows, LANES), F32),
                pltpu.VMEM((2, rows, dim), BF16),
                pltpu.VMEM((2, rows, dim), BF16),
                pltpu.VMEM((n, 8, LANES), F32),
                dma((3,)),
                dma((2, 2 * hops)), dma((2, 2 * hops)), dma((2, 2 * hops)), dma((2, 2 * hops)),
                dma((2, 2 * hops)), dma((2, 2 * hops)), dma((2,)), dma((2,)),
                dma((hops + 1,)), dma((hops + 1,)), dma((hops + 1,)), dma((hops + 1,)),
                dma((2, hops + 1)), dma((2, hops + 1)), dma((2, 2)), dma((2, 2)), dma((n,)), dma((n,)),
            ],
            compiler_params=pltpu.CompilerParams(collective_id=0, has_side_effects=True, vmem_limit_bytes=48 << 20),
            name="leapfrog",
        )(*(pltpu.with_memory_space_constraint(a, pltpu.HBM) for a in
            (positions, velocity, charges.reshape(rows // LANES, LANES))))
        force_zero, force_one = force_zero / dim, force_one / dim
        vel_one = velocity + STEP_SIZE * force_zero
        pos_two = (positions + STEP_SIZE * velocity) + STEP_SIZE * vel_one
        return force_one, energy, pos_two, vel_one + STEP_SIZE * force_one

    return jax.shard_map(local_steps, mesh=mesh, in_specs=(row_spec, row_spec, vec_spec),
                         out_specs=(row_spec, P("sys"), row_spec, row_spec), check_vma=False)
```

```python
import functools

import jax
import jax.numpy as jnp
from jax import lax
from jax.experimental import pallas as pl
from jax.experimental.pallas import tpu as pltpu
from jax.sharding import PartitionSpec as P

MESH = pl.DeviceIdType.MESH
STEP_SIZE = 0.5
LOG2E = 1.4426950408889634
LANES = 128
F32 = jnp.float32
BF16 = jnp.bfloat16


def kernel(n, x0_hbm, v0_hbm, q_hbm, f0_ref, f1_ref, e_ref,
           x0_ref, v0_ref, xg, aux, sc, qc, acc, rho, pout, pin, ebuf, in_sem,
           csend, crecv, tsend, trecv, ssend, srecv, own_send, own_recv,
           asend_r, arecv_r, asend_l, arecv_l, asend_s, arecv_s, psend, precv, esend, erecv):
    rows, dim = x0_ref.shape
    unit = rows // 2
    sub = rows // 4
    chunks = rows // LANES
    hops = n // 4 - 1
    scale = 2.0 * LOG2E / (2.0 * dim)
    me = lax.axis_index("blk")
    right = lax.rem(me + 2, n)
    left = lax.rem(me + n - 2, n)
    sib = me + 1 - 2 * lax.rem(me, 2)
    turn = 1 - 2 * lax.rem(me // 2, 2)

    def side(ev):
        return turn * (1 - 2 * ev)

    def away(dev, ev, hop):
        return lax.rem(dev + n - 2 * side(ev) * hop, n)

    def toward(dev, ev, hop):
        return lax.rem(dev + n + 2 * side(ev) * hop, n)

    def push(ref, send, recv, target, dst=None):
        pltpu.make_async_remote_copy(src_ref=ref, dst_ref=ref if dst is None else dst, send_sem=send, recv_sem=recv,
                                     device_id={"blk": target}, device_id_type=MESH).start()

    def await_recv(ref, send, recv):
        pltpu.make_async_remote_copy(src_ref=ref, dst_ref=ref, send_sem=send, recv_sem=recv,
                                     device_id={"blk": sib}, device_id_type=MESH).wait_recv()

    def await_send(ref, send, recv):
        pltpu.make_async_remote_copy(src_ref=ref, dst_ref=ref, send_sem=send, recv_sem=recv,
                                     device_id={"blk": sib}, device_id_type=MESH).wait_send()

    def span(c):
        return pl.ds(pl.multiple_of(c * LANES, LANES), LANES)

    def piece(ev, src, half):
        return xg.at[ev, src, pl.ds(pl.multiple_of(half * unit, unit), unit), :]

    barrier = pltpu.get_barrier_semaphore()
    for peer in (left, right, sib):
        pl.semaphore_signal(barrier, inc=1, device_id={"blk": peer}, device_id_type=MESH)
    loads = [pltpu.make_async_copy(src, dst, in_sem.at[k])
             for k, (src, dst) in enumerate(((q_hbm, aux.at[me, 0]), (v0_hbm, v0_ref), (x0_hbm, x0_ref)))]
    for load in loads:
        load.start()

    loads[0].wait()
    for c in range(chunks):
        qc[0, c * LANES:(c + 1) * LANES, :] = jnp.broadcast_to(aux[me, 0, c:c + 1, :], (LANES, LANES)).T
    for load in loads[1:]:
        load.wait()

    @pl.loop(0, chunks)
    def _(c):
        xg[1, me, span(c), :] = (x0_ref[span(c), :] + STEP_SIZE * v0_ref[span(c), :]).astype(BF16)

    @pl.loop(0, chunks)
    def _(c):
        xg[0, me, span(c), :] = x0_ref[span(c), :].astype(BF16)

    pl.semaphore_wait(barrier, 3)

    def c_push(ev, src, k, half):
        push(piece(ev, src, half), csend.at[ev, k], crecv.at[ev, k], away(me, ev, 1))

    def t_push(ev, src, k, half):
        push(piece(ev, src, half), tsend.at[ev, k], trecv.at[ev, k], toward(me, ev, 1))

    for ev in (1, 0):
        c_push(ev, me, 0, 0)
        push(xg.at[ev, me], own_send.at[ev], own_recv.at[ev], sib)

    @pl.loop(0, chunks)
    def _(c):
        for ev in (1, 0):
            wide = xg[ev, me, span(c), :].astype(F32)
            norm = jnp.broadcast_to(0.5 * jnp.sum(wide * wide, axis=1, keepdims=True), (LANES, LANES))
            sc[ev, 0, span(c), :] = norm
            aux[me, 1 + ev, pl.ds(c, 1), :] = norm.T[0:1, :]

    acc[...] = jnp.zeros_like(acc)
    rho[...] = jnp.zeros_like(rho)
    push(aux.at[me], asend_s.at[0, 0], arecv_s.at[0, 0], sib)
    push(aux.at[me], asend_r.at[1], arecv_r.at[1], right)
    push(aux.at[me], asend_l.at[1], arecv_l.at[1], left)
    for ev in (1, 0):
        c_push(ev, me, 1, 1)
    for half in (0, 1):
        for ev in (1, 0):
            t_push(ev, me, half, half)

    def pair_unit(ev, party, src, half, own=False):
        mine = toward(me, ev, party)
        xj = xg[ev, src, pl.ds(pl.multiple_of(half * unit, unit), unit), :]
        base = half * (unit // LANES)
        charge = party * (1 + ev)
        if own:
            diff = lax.broadcasted_iota(jnp.int32, (sub, LANES), 0) - lax.broadcasted_iota(jnp.int32, (sub, LANES), 1)
        for r in range(rows // sub):
            rs = pl.ds(r * sub, sub)
            gram = lax.dot_general(xg[ev, mine, rs, :], xj, (((1,), (1,)), ((), ())), preferred_element_type=F32)
            norm_i = sc[ev, party, rs, :]
            q_i = qc[charge, rs, :]
            low, total = [], None
            for c in range(unit // LANES):
                norm_j = aux[src, 1 + ev, pl.ds(base + c, 1), :]
                q_j = aux[src, 0, pl.ds(base + c, 1), :]
                neg = jnp.minimum(gram[:, c * LANES:(c + 1) * LANES] - (norm_i + norm_j), 0.0)
                weight = (q_i * q_j) * jnp.exp2(neg * scale)
                if own:
                    weight = jnp.where(diff == half * unit + (c * LANES - r * sub), 0.0, weight)
                total = weight if total is None else total + weight
                low.append(weight.astype(BF16))
            rho[ev, party, rs, :] += total
            acc[ev, party, rs, :] += jnp.dot(jnp.concatenate(low, axis=1), xj, preferred_element_type=F32)

    for ev in (1, 0):
        for half in (0, 1):
            pair_unit(ev, 0, me, half, own=True)

    await_recv(aux.at[sib], asend_s.at[0, 0], arecv_s.at[0, 0])
    for ev in (1, 0):
        await_recv(xg.at[ev, sib], own_send.at[ev], own_recv.at[ev])

    for ev in (1, 0):
        for half in (0, 1):
            pair_unit(ev, 0, sib, half)

    def table_in(hop):
        for k, (step, send, recv, target) in enumerate(((n - 2 * hop, asend_r, arecv_r, right),
                                                        (2 * hop, asend_l, arecv_l, left))):
            src = lax.rem(me + step, n)
            await_recv(aux.at[src], send.at[hop], recv.at[hop])
            push(aux.at[src], asend_s.at[k, hop], arecv_s.at[k, hop], sib)
            if hop < hops:
                push(aux.at[src], send.at[hop + 1], recv.at[hop + 1], target)

    def table_sib(hop):
        for k, step in enumerate((n - 2 * hop, 2 * hop)):
            await_recv(aux.at[lax.rem(sib + step, n)], asend_s.at[k, hop], arecv_s.at[k, hop])

    def c_take(ev, hop, half):
        k = 2 * (hop - 1) + half
        src = away(me, ev, hop)
        await_recv(piece(ev, src, half), csend.at[ev, k], crecv.at[ev, k])
        push(piece(ev, src, half), ssend.at[ev, k], srecv.at[ev, k], sib)

    def c_sib(ev, hop, half):
        k = 2 * (hop - 1) + half
        await_recv(piece(ev, away(sib, ev, hop), half), ssend.at[ev, k], srecv.at[ev, k])

    def t_take(ev, hop, half):
        k = 2 * (hop - 1) + half
        src = toward(me, ev, hop)
        await_recv(piece(ev, src, half), tsend.at[ev, k], trecv.at[ev, k])
        c_push(ev, src, 2 * hop + half, half)

    @pl.loop(0, 2)
    def _(half):
        for ev in (1, 0):
            c_take(ev, 1, half)
            t_push(ev, away(me, ev, 1), 2 + half, half)

        @pl.when(half == 0)
        def _():
            table_in(1)

        for ev in (1, 0):
            pair_unit(ev, 0, away(me, ev, 1), half)

        for ev in (1, 0):
            c_sib(ev, 1, half)

        @pl.when(half == 0)
        def _():
            table_sib(1)

        for ev in (1, 0):
            pair_unit(ev, 0, away(sib, ev, 1), half)

    for half in (0, 1):
        for ev in (1, 0):
            t_take(ev, 1, half)
    table_in(2)

    for ev in (1, 0):
        mate = toward(me, ev, 1)

        @pl.loop(0, chunks)
        def _(c):
            sc[ev, 1, span(c), :] = jnp.broadcast_to(aux[mate, 1 + ev, pl.ds(c, 1), :], (LANES, LANES)).T
            qc[1 + ev, span(c), :] = jnp.broadcast_to(aux[mate, 0, pl.ds(c, 1), :], (LANES, LANES)).T

    @pl.loop(0, 4)
    def _(j):
        @pl.when(j == 2)
        def _():
            for ev in (1, 0):
                t_take(ev, 2, 0)

        who = lax.rem(j, 2)
        for ev in (1, 0):
            for half in (0, 1):
                pair_unit(ev, 1, away(me + who * (sib - me), ev, j // 2), half)

    for ev in (1, 0):
        t_take(ev, 2, 1)

    last = 2 * hops - 1

    @pl.loop(2, last)
    def _(k):
        hop = 1 + k // 2
        half = lax.rem(k, 2)
        for ev in (1, 0):
            c_take(ev, hop, half)

        @pl.when(k == last - 1)
        def _():
            table_in(3)

        @pl.loop(0, 2)
        def _(j):
            @pl.when(j == 1)
            def _():
                for ev in (1, 0):
                    c_sib(ev, hop, half)

                @pl.when(k == 2)
                def _():
                    table_sib(2)

                @pl.when(k == last - 1)
                def _():
                    table_sib(3)

            for ev in (1, 0):
                for party in (1, 0):
                    pair_unit(ev, party, away(me + j * (sib - me), ev, hop), half)

    for ev in (1, 0):
        c_take(ev, hops, 1)

    def force(ev, party, c):
        held = jnp.sum(rho[ev, party, span(c), :], axis=1, keepdims=True)
        return held * xg[ev, toward(me, ev, party), span(c), :].astype(F32) - acc[ev, party, span(c), :]

    def part(ref, ev, half):
        return ref.at[ev, pl.ds(half * unit, unit), :]

    def give(ev, half):
        push(part(pout, ev, half), psend.at[ev, half], precv.at[ev, half], toward(me, ev, 1), part(pin, ev, half))

    @pl.loop(0, 2)
    def _(j):
        @pl.when(j == 1)
        def _():
            for ev in (1, 0):
                c_sib(ev, hops, 1)

        for ev in (1, 0):
            pair_unit(ev, 1, away(me + j * (sib - me), ev, hops), 1)

    for ev in (1, 0):
        @pl.loop(0, chunks)
        def _(c):
            pout[ev, span(c), :] = force(ev, 1, c).astype(BF16)

        give(ev, 0)

    for dev in (me, sib):
        pair_unit(1, 0, away(dev, 1, hops), 1)

    ebuf[me] = jnp.broadcast_to(0.5 * jnp.sum(rho[1, 0] + rho[1, 1], keepdims=True), ebuf.shape[1:])

    @pl.loop(0, chunks)
    def _(c):
        f1_ref[span(c), :] = force(1, 0, c)

    @pl.loop(1, n)
    def _(k):
        peer = lax.rem(me + k, n)
        push(ebuf.at[me], esend.at[peer], erecv.at[me], peer)

    give(1, 1)
    give(0, 1)
    for dev in (me, sib):
        pair_unit(0, 0, away(dev, 0, hops), 1)

    @pl.loop(0, chunks)
    def _(c):
        f0_ref[span(c), :] = force(0, 0, c)

    for half in (0, 1):
        for ev, out_ref in ((1, f1_ref), (0, f0_ref)):
            await_recv(part(pin, ev, half), psend.at[ev, half], precv.at[ev, half])

            @pl.loop(half * (chunks // 2), (half + 1) * (chunks // 2))
            def _(c):
                out_ref[span(c), :] += pin[ev, span(c), :].astype(F32)

    @pl.loop(1, n)
    def _(p):
        peer = lax.rem(me + p, n)
        await_recv(ebuf.at[peer], esend.at[peer], erecv.at[peer])
        await_send(ebuf.at[me], esend.at[peer], erecv.at[me])

    e_ref[0] = jnp.sum(jnp.sum(ebuf[...], axis=0)[0:1, 0:1])

    for ev in (0, 1):
        @pl.loop(0, 2 * hops)
        def _(k):
            await_send(piece(ev, me, 0), csend.at[ev, k], crecv.at[ev, k])
            await_send(piece(ev, me, 0), ssend.at[ev, k], srecv.at[ev, k])

        @pl.loop(0, 2 * hops - 2)
        def _(k):
            await_send(piece(ev, me, 0), tsend.at[ev, k], trecv.at[ev, k])

        await_send(xg.at[ev, me], own_send.at[ev], own_recv.at[ev])
        for half in (0, 1):
            await_send(part(pout, ev, half), psend.at[ev, half], precv.at[ev, half])

    table = aux.at[me]
    await_send(table, asend_s.at[0, 0], arecv_s.at[0, 0])
    for hop in range(1, hops + 1):
        await_send(table, asend_r.at[hop], arecv_r.at[hop])
        await_send(table, asend_l.at[hop], arecv_l.at[hop])
        await_send(table, asend_s.at[0, hop], arecv_s.at[0, hop])
        await_send(table, asend_s.at[1, hop], arecv_s.at[1, hop])


def solution(mesh):
    n = mesh.shape["blk"]
    row_spec = P(("sys", "blk"), None)
    vec_spec = P(("sys", "blk"))

    def local_steps(positions, velocity, charges):
        rows, dim = positions.shape
        hops = n // 4 - 1
        dma = pltpu.SemaphoreType.DMA
        whole = pl.BlockSpec(memory_space=pltpu.VMEM)
        flat = jax.ShapeDtypeStruct((rows, dim), F32)
        force_zero, force_one, energy = pl.pallas_call(
            functools.partial(kernel, n),
            out_shape=(flat, flat, jax.ShapeDtypeStruct((1,), F32)),
            in_specs=[pl.BlockSpec(memory_space=pltpu.HBM)] * 3,
            out_specs=(whole, whole, pl.BlockSpec(memory_space=pltpu.SMEM)),
            scratch_shapes=[
                pltpu.VMEM((rows, dim), F32),
                pltpu.VMEM((rows, dim), F32),
                pltpu.VMEM((2, n, rows, dim), BF16),
                pltpu.VMEM((n, 3, rows // LANES, LANES), F32),
                pltpu.VMEM((2, 2, rows, LANES), F32),
                pltpu.VMEM((3, rows, LANES), F32),
                pltpu.VMEM((2, 2, rows, dim), F32),
                pltpu.VMEM((2, 2, rows, LANES), F32),
                pltpu.VMEM((2, rows, dim), BF16),
                pltpu.VMEM((2, rows, dim), BF16),
                pltpu.VMEM((n, 8, LANES), F32),
                dma((3,)),
                dma((2, 2 * hops)), dma((2, 2 * hops)), dma((2, 2 * hops)), dma((2, 2 * hops)),
                dma((2, 2 * hops)), dma((2, 2 * hops)), dma((2,)), dma((2,)),
                dma((hops + 1,)), dma((hops + 1,)), dma((hops + 1,)), dma((hops + 1,)),
                dma((2, hops + 1)), dma((2, hops + 1)), dma((2, 2)), dma((2, 2)), dma((n,)), dma((n,)),
            ],
            compiler_params=pltpu.CompilerParams(collective_id=0, has_side_effects=True, vmem_limit_bytes=48 << 20),
            name="leapfrog",
        )(*(pltpu.with_memory_space_constraint(a, pltpu.HBM) for a in
            (positions, velocity, charges.reshape(rows // LANES, LANES))))
        force_zero, force_one = force_zero / dim, force_one / dim
        vel_one = velocity + STEP_SIZE * force_zero
        pos_two = (positions + STEP_SIZE * velocity) + STEP_SIZE * vel_one
        return force_one, energy, pos_two, vel_one + STEP_SIZE * force_one

    return jax.shard_map(local_steps, mesh=mesh, in_specs=(row_spec, row_spec, vec_spec),
                         out_specs=(row_spec, P("sys"), row_spec, row_spec), check_vma=False)
```

```python
import functools

import jax
import jax.numpy as jnp
from jax import lax
from jax.experimental import pallas as pl
from jax.experimental.pallas import tpu as pltpu
from jax.sharding import PartitionSpec as P

MESH = pl.DeviceIdType.MESH
STEP_SIZE = 0.5
LOG2E = 1.4426950408889634
LANES = 128
F32 = jnp.float32
BF16 = jnp.bfloat16


def kernel(n, x0_hbm, v0_hbm, q_hbm, f0_ref, f1_ref, e_ref,
           x0_ref, v0_ref, xg, aux, sc, qc, acc, rho, pout, pin, ebuf, in_sem,
           csend, crecv, tsend, trecv, ssend, srecv, own_send, own_recv,
           asend_r, arecv_r, asend_l, arecv_l, asend_s, arecv_s, psend, precv, esend, erecv):
    rows, dim = x0_ref.shape
    unit = rows // 2
    sub = rows // 4
    chunks = rows // LANES
    hops = n // 4 - 1
    scale = 2.0 * LOG2E / (2.0 * dim)
    me = lax.axis_index("blk")
    right = lax.rem(me + 2, n)
    left = lax.rem(me + n - 2, n)
    sib = me + 1 - 2 * lax.rem(me, 2)
    turn = 1 - 2 * lax.rem(me // 2, 2)

    def side(ev):
        return turn * (1 - 2 * ev)

    def away(dev, ev, hop):
        return lax.rem(dev + n - 2 * side(ev) * hop, n)

    def toward(dev, ev, hop):
        return lax.rem(dev + n + 2 * side(ev) * hop, n)

    def push(ref, send, recv, target, dst=None):
        pltpu.make_async_remote_copy(src_ref=ref, dst_ref=ref if dst is None else dst, send_sem=send, recv_sem=recv,
                                     device_id={"blk": target}, device_id_type=MESH).start()

    def await_recv(ref, send, recv):
        pltpu.make_async_remote_copy(src_ref=ref, dst_ref=ref, send_sem=send, recv_sem=recv,
                                     device_id={"blk": sib}, device_id_type=MESH).wait_recv()

    def await_send(ref, send, recv):
        pltpu.make_async_remote_copy(src_ref=ref, dst_ref=ref, send_sem=send, recv_sem=recv,
                                     device_id={"blk": sib}, device_id_type=MESH).wait_send()

    def span(c):
        return pl.ds(pl.multiple_of(c * LANES, LANES), LANES)

    def piece(ev, src, half):
        return xg.at[ev, src, pl.ds(pl.multiple_of(half * unit, unit), unit), :]

    barrier = pltpu.get_barrier_semaphore()
    for peer in (left, right, sib):
        pl.semaphore_signal(barrier, inc=1, device_id={"blk": peer}, device_id_type=MESH)
    loads = [pltpu.make_async_copy(src, dst, in_sem.at[k])
             for k, (src, dst) in enumerate(((q_hbm, aux.at[me, 0]), (v0_hbm, v0_ref), (x0_hbm, x0_ref)))]
    for load in loads:
        load.start()

    loads[0].wait()
    for c in range(chunks):
        qc[0, c * LANES:(c + 1) * LANES, :] = jnp.broadcast_to(aux[me, 0, c:c + 1, :], (LANES, LANES)).T
    for load in loads[1:]:
        load.wait()

    @pl.loop(0, chunks)
    def _(c):
        xg[1, me, span(c), :] = (x0_ref[span(c), :] + STEP_SIZE * v0_ref[span(c), :]).astype(BF16)

    @pl.loop(0, chunks)
    def _(c):
        xg[0, me, span(c), :] = x0_ref[span(c), :].astype(BF16)

    pl.semaphore_wait(barrier, 3)

    def c_push(ev, src, k, half):
        push(piece(ev, src, half), csend.at[ev, k], crecv.at[ev, k], away(me, ev, 1))

    def t_push(ev, src, k, half):
        push(piece(ev, src, half), tsend.at[ev, k], trecv.at[ev, k], toward(me, ev, 1))

    for ev in (1, 0):
        t_push(ev, me, 0, 0)
        push(xg.at[ev, me], own_send.at[ev], own_recv.at[ev], sib)

    @pl.loop(0, chunks)
    def _(c):
        for ev in (1, 0):
            wide = xg[ev, me, span(c), :].astype(F32)
            norm = jnp.broadcast_to(0.5 * jnp.sum(wide * wide, axis=1, keepdims=True), (LANES, LANES))
            sc[ev, 0, span(c), :] = norm
            aux[me, 1 + ev, pl.ds(c, 1), :] = norm.T[0:1, :]

    acc[...] = jnp.zeros_like(acc)
    rho[...] = jnp.zeros_like(rho)
    push(aux.at[me], asend_s.at[0, 0], arecv_s.at[0, 0], sib)
    push(aux.at[me], asend_r.at[1], arecv_r.at[1], right)
    push(aux.at[me], asend_l.at[1], arecv_l.at[1], left)
    for ev in (1, 0):
        t_push(ev, me, 1, 1)
    for half in (0, 1):
        for ev in (1, 0):
            c_push(ev, me, half, half)

    def pair_rows(ev, party, src, half, start, count, own=False):
        xj = xg[ev, src, pl.ds(pl.multiple_of(half * unit, unit), unit), :]
        base = half * (unit // LANES)
        rs = pl.ds(start, count)
        gram = lax.dot_general(xg[ev, toward(me, ev, party), rs, :], xj, (((1,), (1,)), ((), ())),
                               preferred_element_type=F32)
        norm_i = sc[ev, party, rs, :]
        q_i = qc[party * (1 + ev), rs, :]
        if own:
            diff = lax.broadcasted_iota(jnp.int32, (count, LANES), 0) - lax.broadcasted_iota(jnp.int32, (count, LANES), 1)
        low, total = [], None
        for c in range(unit // LANES):
            norm_j = aux[src, 1 + ev, pl.ds(base + c, 1), :]
            q_j = aux[src, 0, pl.ds(base + c, 1), :]
            neg = jnp.minimum(gram[:, c * LANES:(c + 1) * LANES] - (norm_i + norm_j), 0.0)
            weight = (q_i * q_j) * jnp.exp2(neg * scale)
            if own:
                weight = jnp.where(diff == half * unit + (c * LANES - start), 0.0, weight)
            total = weight if total is None else total + weight
            low.append(weight.astype(BF16))
        rho[ev, party, rs, :] += total
        acc[ev, party, rs, :] += jnp.dot(jnp.concatenate(low, axis=1), xj, preferred_element_type=F32)

    def pair_unit(ev, party, src, half, own=False):
        for r in range(rows // sub):
            pair_rows(ev, party, src, half, r * sub, sub, own)

    await_recv(aux.at[sib], asend_s.at[0, 0], arecv_s.at[0, 0])
    for ev in (1, 0):
        await_recv(xg.at[ev, sib], own_send.at[ev], own_recv.at[ev])

    @pl.loop(0, 2)
    def _(ev):
        for src in (me, sib):
            for half in (0, 1):
                pair_unit(ev, 0, src, half, own=src is me)

    def table_in(hop):
        for k, (step, send, recv, target) in enumerate(((n - 2 * hop, asend_r, arecv_r, right),
                                                        (2 * hop, asend_l, arecv_l, left))):
            src = lax.rem(me + step, n)
            await_recv(aux.at[src], send.at[hop], recv.at[hop])
            push(aux.at[src], asend_s.at[k, hop], arecv_s.at[k, hop], sib)
            if hop < hops:
                push(aux.at[src], send.at[hop + 1], recv.at[hop + 1], target)

    def table_sib(hop):
        for k, step in enumerate((n - 2 * hop, 2 * hop)):
            await_recv(aux.at[lax.rem(sib + step, n)], asend_s.at[k, hop], arecv_s.at[k, hop])

    def c_take(ev, hop, half):
        k = 2 * (hop - 1) + half
        src = away(me, ev, hop)
        await_recv(piece(ev, src, half), csend.at[ev, k], crecv.at[ev, k])
        push(piece(ev, src, half), ssend.at[ev, k], srecv.at[ev, k], sib)

    def c_sib(ev, hop, half):
        k = 2 * (hop - 1) + half
        await_recv(piece(ev, away(sib, ev, hop), half), ssend.at[ev, k], srecv.at[ev, k])

    def t_take(ev, hop, half):
        k = 2 * (hop - 1) + half
        src = toward(me, ev, hop)
        await_recv(piece(ev, src, half), tsend.at[ev, k], trecv.at[ev, k])
        c_push(ev, src, 2 * hop + half, half)

    for half in (0, 1):
        for ev in (1, 0):
            t_take(ev, 1, half)
        if half == 0:
            table_in(1)

    for ev in (1, 0):
        mate = toward(me, ev, 1)

        @pl.loop(0, chunks)
        def _(c):
            sc[ev, 1, span(c), :] = jnp.broadcast_to(aux[mate, 1 + ev, pl.ds(c, 1), :], (LANES, LANES)).T
            qc[1 + ev, span(c), :] = jnp.broadcast_to(aux[mate, 0, pl.ds(c, 1), :], (LANES, LANES)).T

    @pl.loop(0, 2)
    def _(ev):
        for src in (me, sib):
            for half in (0, 1):
                pair_unit(ev, 1, src, half)

    last = 2 * hops - 2

    @pl.loop(0, last)
    def _(k):
        hop = 1 + k // 2
        half = lax.rem(k, 2)
        for ev in (1, 0):
            c_take(ev, hop, half)

            @pl.when(hop == 1)
            def _():
                t_push(ev, away(me, ev, 1), 2 + half, half)

        @pl.when(k == 0)
        def _():
            table_in(2)

        @pl.loop(0, 2)
        def _(ev):
            c_sib(ev, hop, half)

            @pl.when((k == 0) & (ev == 0))
            def _():
                table_sib(1)

            @pl.when((k == 2) & (ev == 0))
            def _():
                table_sib(2)

            for party in (1, 0):
                for dev in (me, sib):
                    pair_unit(ev, party, away(dev, ev, hop), half)

        @pl.when((k == 1) | (k == 2))
        def _():
            for ev in (1, 0):
                t_take(ev, 2, k - 1)

    for ev in (1, 0):
        c_take(ev, hops, 0)
    table_in(3)
    for ev in (1, 0):
        c_sib(ev, hops, 0)
    table_sib(3)

    for ev in (1, 0):
        for dev in (me, sib):
            pair_unit(ev, 1, away(dev, ev, hops), 0)

    def force(ev, party, c):
        held = jnp.sum(rho[ev, party, span(c), :], axis=1, keepdims=True)
        return held * xg[ev, toward(me, ev, party), span(c), :].astype(F32) - acc[ev, party, span(c), :]

    for ev in (1, 0):
        c_take(ev, hops, 1)
    for ev in (1, 0):
        c_sib(ev, hops, 1)

    def part(ref, ev, r):
        return ref.at[ev, pl.ds(pl.multiple_of(r * sub, sub), sub), :]

    def give(ev, r):
        push(part(pout, ev, r), psend.at[ev, r], precv.at[ev, r], toward(me, ev, 1), part(pin, ev, r))

    parts = rows // sub

    @pl.loop(0, 2 * parts)
    def _(j):
        ev = 1 - lax.rem(j, 2)
        r = j // 2
        for dev in (me, sib):
            pair_rows(ev, 1, away(dev, ev, hops), 1, pl.multiple_of(r * sub, sub), sub)

        @pl.when((j > 0) & (j < 2 * parts - 1))
        def _():
            give(1 - ev, (j - 1) // 2)

        for c in range(sub // LANES):
            at = r * (sub // LANES) + c
            pout[ev, span(at), :] = force(ev, 1, at).astype(BF16)

    def own_rows(ev, out_ref):
        for half in (0, 1):
            for dev in (me, sib):
                pair_unit(ev, 0, away(dev, ev, hops), half)

        @pl.loop(0, chunks)
        def _(c):
            out_ref[span(c), :] = force(ev, 0, c)

    own_rows(1, f1_ref)
    ebuf[me] = jnp.broadcast_to(0.5 * jnp.sum(rho[1, 0] + rho[1, 1], keepdims=True), ebuf.shape[1:])
    give(1, parts - 1)

    @pl.loop(1, n)
    def _(k):
        peer = lax.rem(me + k, n)
        push(ebuf.at[me], esend.at[peer], erecv.at[me], peer)

    give(0, parts - 1)
    own_rows(0, f0_ref)

    for r in range(parts):
        for ev, out_ref in ((1, f1_ref), (0, f0_ref)):
            await_recv(part(pin, ev, r), psend.at[ev, r], precv.at[ev, r])
            for c in range(sub // LANES):
                at = r * (sub // LANES) + c
                out_ref[span(at), :] += pin[ev, span(at), :].astype(F32)

    @pl.loop(1, n)
    def _(p):
        peer = lax.rem(me + p, n)
        await_recv(ebuf.at[peer], esend.at[peer], erecv.at[peer])
        await_send(ebuf.at[me], esend.at[peer], erecv.at[me])

    e_ref[0] = jnp.sum(jnp.sum(ebuf[...], axis=0)[0:1, 0:1])

    for ev in (0, 1):
        @pl.loop(0, 2 * hops)
        def _(k):
            await_send(piece(ev, me, 0), csend.at[ev, k], crecv.at[ev, k])
            await_send(piece(ev, me, 0), ssend.at[ev, k], srecv.at[ev, k])

        @pl.loop(0, 2 * hops - 2)
        def _(k):
            await_send(piece(ev, me, 0), tsend.at[ev, k], trecv.at[ev, k])

        await_send(xg.at[ev, me], own_send.at[ev], own_recv.at[ev])
        for r in range(parts):
            await_send(part(pout, ev, r), psend.at[ev, r], precv.at[ev, r])

    table = aux.at[me]
    await_send(table, asend_s.at[0, 0], arecv_s.at[0, 0])
    for hop in range(1, hops + 1):
        await_send(table, asend_r.at[hop], arecv_r.at[hop])
        await_send(table, asend_l.at[hop], arecv_l.at[hop])
        await_send(table, asend_s.at[0, hop], arecv_s.at[0, hop])
        await_send(table, asend_s.at[1, hop], arecv_s.at[1, hop])


def solution(mesh):
    n = mesh.shape["blk"]
    row_spec = P(("sys", "blk"), None)
    vec_spec = P(("sys", "blk"))

    def local_steps(positions, velocity, charges):
        rows, dim = positions.shape
        hops = n // 4 - 1
        dma = pltpu.SemaphoreType.DMA
        whole = pl.BlockSpec(memory_space=pltpu.VMEM)
        flat = jax.ShapeDtypeStruct((rows, dim), F32)
        force_zero, force_one, energy = pl.pallas_call(
            functools.partial(kernel, n),
            out_shape=(flat, flat, jax.ShapeDtypeStruct((1,), F32)),
            in_specs=[pl.BlockSpec(memory_space=pltpu.HBM)] * 3,
            out_specs=(whole, whole, pl.BlockSpec(memory_space=pltpu.SMEM)),
            scratch_shapes=[
                pltpu.VMEM((rows, dim), F32),
                pltpu.VMEM((rows, dim), F32),
                pltpu.VMEM((2, n, rows, dim), BF16),
                pltpu.VMEM((n, 3, rows // LANES, LANES), F32),
                pltpu.VMEM((2, 2, rows, LANES), F32),
                pltpu.VMEM((3, rows, LANES), F32),
                pltpu.VMEM((2, 2, rows, dim), F32),
                pltpu.VMEM((2, 2, rows, LANES), F32),
                pltpu.VMEM((2, rows, dim), BF16),
                pltpu.VMEM((2, rows, dim), BF16),
                pltpu.VMEM((n, 8, LANES), F32),
                dma((3,)),
                dma((2, 2 * hops)), dma((2, 2 * hops)), dma((2, 2 * hops)), dma((2, 2 * hops)),
                dma((2, 2 * hops)), dma((2, 2 * hops)), dma((2,)), dma((2,)),
                dma((hops + 1,)), dma((hops + 1,)), dma((hops + 1,)), dma((hops + 1,)),
                dma((2, hops + 1)), dma((2, hops + 1)), dma((2, 4)), dma((2, 4)), dma((n,)), dma((n,)),
            ],
            compiler_params=pltpu.CompilerParams(collective_id=0, has_side_effects=True, vmem_limit_bytes=48 << 20),
            name="leapfrog",
        )(*(pltpu.with_memory_space_constraint(a, pltpu.HBM) for a in
            (positions, velocity, charges.reshape(rows // LANES, LANES))))
        force_zero, force_one = force_zero / dim, force_one / dim
        vel_one = velocity + STEP_SIZE * force_zero
        pos_two = (positions + STEP_SIZE * velocity) + STEP_SIZE * vel_one
        return force_one, energy, pos_two, vel_one + STEP_SIZE * force_one

    return jax.shard_map(local_steps, mesh=mesh, in_specs=(row_spec, row_spec, vec_spec),
                         out_specs=(row_spec, P("sys"), row_spec, row_spec), check_vma=False)
```

```python
import functools

import jax
import jax.numpy as jnp
from jax import lax
from jax.experimental import pallas as pl
from jax.experimental.pallas import tpu as pltpu
from jax.sharding import PartitionSpec as P

MESH = pl.DeviceIdType.MESH
STEP_SIZE = 0.5
LOG2E = 1.4426950408889634
LANES = 128
F32 = jnp.float32
BF16 = jnp.bfloat16


def kernel(n, x0_hbm, v0_hbm, q_hbm, f0_ref, f1_ref, e_ref,
           x0_ref, v0_ref, xg, aux, sc, qc, acc, rho, pout, pin, ebuf, in_sem,
           csend, crecv, tsend, trecv, ssend, srecv, own_send, own_recv,
           asend_r, arecv_r, asend_l, arecv_l, asend_s, arecv_s, psend, precv, esend, erecv):
    rows, dim = x0_ref.shape
    unit = rows // 2
    sub = rows // 4
    chunks = rows // LANES
    hops = n // 4 - 1
    scale = 2.0 * LOG2E / (2.0 * dim)
    me = lax.axis_index("blk")
    right = lax.rem(me + 2, n)
    left = lax.rem(me + n - 2, n)
    sib = me + 1 - 2 * lax.rem(me, 2)
    turn = 1 - 2 * lax.rem(me // 2, 2)

    def side(ev):
        return turn * (1 - 2 * ev)

    def away(dev, ev, hop):
        return lax.rem(dev + n - 2 * side(ev) * hop, n)

    def toward(dev, ev, hop):
        return lax.rem(dev + n + 2 * side(ev) * hop, n)

    def push(ref, send, recv, target, dst=None):
        pltpu.make_async_remote_copy(src_ref=ref, dst_ref=ref if dst is None else dst, send_sem=send, recv_sem=recv,
                                     device_id={"blk": target}, device_id_type=MESH).start()

    def await_recv(ref, send, recv):
        pltpu.make_async_remote_copy(src_ref=ref, dst_ref=ref, send_sem=send, recv_sem=recv,
                                     device_id={"blk": sib}, device_id_type=MESH).wait_recv()

    def await_send(ref, send, recv):
        pltpu.make_async_remote_copy(src_ref=ref, dst_ref=ref, send_sem=send, recv_sem=recv,
                                     device_id={"blk": sib}, device_id_type=MESH).wait_send()

    def span(c):
        return pl.ds(pl.multiple_of(c * LANES, LANES), LANES)

    def piece(ev, src, half):
        return xg.at[ev, src, pl.ds(pl.multiple_of(half * unit, unit), unit), :]

    barrier = pltpu.get_barrier_semaphore()
    for peer in (left, right, sib):
        pl.semaphore_signal(barrier, inc=1, device_id={"blk": peer}, device_id_type=MESH)
    loads = [pltpu.make_async_copy(src, dst, in_sem.at[k])
             for k, (src, dst) in enumerate(((q_hbm, aux.at[me, 0]), (v0_hbm, v0_ref), (x0_hbm, x0_ref)))]
    for load in loads:
        load.start()

    loads[0].wait()
    for c in range(chunks):
        qc[0, c * LANES:(c + 1) * LANES, :] = jnp.broadcast_to(aux[me, 0, c:c + 1, :], (LANES, LANES)).T
    for load in loads[1:]:
        load.wait()

    @pl.loop(0, chunks)
    def _(c):
        xg[1, me, span(c), :] = (x0_ref[span(c), :] + STEP_SIZE * v0_ref[span(c), :]).astype(BF16)

    @pl.loop(0, chunks)
    def _(c):
        xg[0, me, span(c), :] = x0_ref[span(c), :].astype(BF16)

    pl.semaphore_wait(barrier, 3)

    def c_push(ev, src, k, half):
        push(piece(ev, src, half), csend.at[ev, k], crecv.at[ev, k], away(me, ev, 1))

    def t_push(ev, src, k, half):
        push(piece(ev, src, half), tsend.at[ev, k], trecv.at[ev, k], toward(me, ev, 1))

    for ev in (1, 0):
        t_push(ev, me, 0, 0)
        push(xg.at[ev, me], own_send.at[ev], own_recv.at[ev], sib)

    @pl.loop(0, chunks)
    def _(c):
        for ev in (1, 0):
            wide = xg[ev, me, span(c), :].astype(F32)
            norm = jnp.broadcast_to(0.5 * jnp.sum(wide * wide, axis=1, keepdims=True), (LANES, LANES))
            sc[ev, 0, span(c), :] = norm
            aux[me, 1 + ev, pl.ds(c, 1), :] = norm.T[0:1, :]

    acc[...] = jnp.zeros_like(acc)
    rho[...] = jnp.zeros_like(rho)
    push(aux.at[me], asend_s.at[0, 0], arecv_s.at[0, 0], sib)
    push(aux.at[me], asend_r.at[1], arecv_r.at[1], right)
    push(aux.at[me], asend_l.at[1], arecv_l.at[1], left)
    for ev in (1, 0):
        t_push(ev, me, 1, 1)
    for half in (0, 1):
        for ev in (1, 0):
            c_push(ev, me, half, half)

    def pair_rows(ev, party, src, half, start, count, own=False):
        xj = xg[ev, src, pl.ds(pl.multiple_of(half * unit, unit), unit), :]
        base = half * (unit // LANES)
        rs = pl.ds(start, count)
        gram = lax.dot_general(xg[ev, toward(me, ev, party), rs, :], xj, (((1,), (1,)), ((), ())),
                               preferred_element_type=F32)
        norm_i = sc[ev, party, rs, :]
        q_i = qc[party * (1 + ev), rs, :]
        if own:
            diff = lax.broadcasted_iota(jnp.int32, (count, LANES), 0) - lax.broadcasted_iota(jnp.int32, (count, LANES), 1)
        low, total = [], None
        for c in range(unit // LANES):
            norm_j = aux[src, 1 + ev, pl.ds(base + c, 1), :]
            q_j = aux[src, 0, pl.ds(base + c, 1), :]
            neg = jnp.minimum(gram[:, c * LANES:(c + 1) * LANES] - (norm_i + norm_j), 0.0)
            weight = (q_i * q_j) * jnp.exp2(neg * scale)
            if own:
                weight = jnp.where(diff == half * unit + (c * LANES - start), 0.0, weight)
            total = weight if total is None else total + weight
            low.append(weight.astype(BF16))
        rho[ev, party, rs, :] += total
        acc[ev, party, rs, :] += jnp.dot(jnp.concatenate(low, axis=1), xj, preferred_element_type=F32)

    def pair_unit(ev, party, src, half, own=False):
        for r in range(rows // sub):
            pair_rows(ev, party, src, half, r * sub, sub, own)

    await_recv(aux.at[sib], asend_s.at[0, 0], arecv_s.at[0, 0])
    for ev in (1, 0):
        await_recv(xg.at[ev, sib], own_send.at[ev], own_recv.at[ev])

    @pl.loop(0, 2)
    def _(ev):
        for src in (me, sib):
            for half in (0, 1):
                pair_unit(ev, 0, src, half, own=src is me)

    def table_in(hop):
        for k, (step, send, recv, target) in enumerate(((n - 2 * hop, asend_r, arecv_r, right),
                                                        (2 * hop, asend_l, arecv_l, left))):
            src = lax.rem(me + step, n)
            await_recv(aux.at[src], send.at[hop], recv.at[hop])
            push(aux.at[src], asend_s.at[k, hop], arecv_s.at[k, hop], sib)
            if hop < hops:
                push(aux.at[src], send.at[hop + 1], recv.at[hop + 1], target)

    def table_sib(hop):
        for k, step in enumerate((n - 2 * hop, 2 * hop)):
            await_recv(aux.at[lax.rem(sib + step, n)], asend_s.at[k, hop], arecv_s.at[k, hop])

    def c_take(ev, hop, half):
        k = 2 * (hop - 1) + half
        src = away(me, ev, hop)
        await_recv(piece(ev, src, half), csend.at[ev, k], crecv.at[ev, k])
        push(piece(ev, src, half), ssend.at[ev, k], srecv.at[ev, k], sib)

    def c_sib(ev, hop, half):
        k = 2 * (hop - 1) + half
        await_recv(piece(ev, away(sib, ev, hop), half), ssend.at[ev, k], srecv.at[ev, k])

    def t_take(ev, hop, half):
        k = 2 * (hop - 1) + half
        src = toward(me, ev, hop)
        await_recv(piece(ev, src, half), tsend.at[ev, k], trecv.at[ev, k])
        c_push(ev, src, 2 * hop + half, half)

    for half in (0, 1):
        for ev in (1, 0):
            t_take(ev, 1, half)
        if half == 0:
            table_in(1)

    for ev in (1, 0):
        mate = toward(me, ev, 1)

        @pl.loop(0, chunks)
        def _(c):
            sc[ev, 1, span(c), :] = jnp.broadcast_to(aux[mate, 1 + ev, pl.ds(c, 1), :], (LANES, LANES)).T
            qc[1 + ev, span(c), :] = jnp.broadcast_to(aux[mate, 0, pl.ds(c, 1), :], (LANES, LANES)).T

    @pl.loop(0, 2)
    def _(ev):
        for src in (me, sib):
            for half in (0, 1):
                pair_unit(ev, 1, src, half)

    last = 2 * hops - 2

    @pl.loop(0, last)
    def _(k):
        hop = 1 + k // 2
        half = lax.rem(k, 2)
        for ev in (1, 0):
            c_take(ev, hop, half)

            @pl.when(hop == 1)
            def _():
                t_push(ev, away(me, ev, 1), 2 + half, half)

        @pl.when(k == 0)
        def _():
            table_in(2)

        @pl.loop(0, 2)
        def _(ev):
            c_sib(ev, hop, half)

            @pl.when((k == 0) & (ev == 0))
            def _():
                table_sib(1)

            @pl.when((k == 2) & (ev == 0))
            def _():
                table_sib(2)

            for party in (1, 0):
                for dev in (me, sib):
                    pair_unit(ev, party, away(dev, ev, hop), half)

        @pl.when((k == 1) | (k == 2))
        def _():
            for ev in (1, 0):
                t_take(ev, 2, k - 1)

    for ev in (1, 0):
        c_take(ev, hops, 0)
    table_in(3)
    for ev in (1, 0):
        c_sib(ev, hops, 0)
    table_sib(3)

    for ev in (1, 0):
        for dev in (me, sib):
            pair_unit(ev, 1, away(dev, ev, hops), 0)

    def force(ev, party, c):
        held = jnp.sum(rho[ev, party, span(c), :], axis=1, keepdims=True)
        return held * xg[ev, toward(me, ev, party), span(c), :].astype(F32) - acc[ev, party, span(c), :]

    for ev in (1, 0):
        c_take(ev, hops, 1)
    for ev in (1, 0):
        c_sib(ev, hops, 1)

    def part(ref, ev, r):
        return ref.at[ev, pl.ds(pl.multiple_of(r * sub, sub), sub), :]

    def give(ev, r):
        push(part(pout, ev, r), psend.at[ev, r], precv.at[ev, r], toward(me, ev, 1), part(pin, ev, r))

    parts = rows // sub

    @pl.loop(0, 2 * parts)
    def _(j):
        ev = 1 - lax.rem(j, 2)
        r = j // 2
        for dev in (me, sib):
            pair_rows(ev, 1, away(dev, ev, hops), 1, pl.multiple_of(r * sub, sub), sub)

        @pl.when(j > 0)
        def _():
            give(1 - ev, (j - 1) // 2)

        for c in range(sub // LANES):
            at = r * (sub // LANES) + c
            pout[ev, span(at), :] = force(ev, 1, at).astype(BF16)

    for ev in (0, 1):
        @pl.loop(0, 2 * hops)
        def _(k):
            await_send(piece(ev, me, 0), csend.at[ev, k], crecv.at[ev, k])
            await_send(piece(ev, me, 0), ssend.at[ev, k], srecv.at[ev, k])

        @pl.loop(0, 2 * hops - 2)
        def _(k):
            await_send(piece(ev, me, 0), tsend.at[ev, k], trecv.at[ev, k])

        await_send(xg.at[ev, me], own_send.at[ev], own_recv.at[ev])

    table = aux.at[me]
    await_send(table, asend_s.at[0, 0], arecv_s.at[0, 0])
    for hop in range(1, hops + 1):
        await_send(table, asend_r.at[hop], arecv_r.at[hop])
        await_send(table, asend_l.at[hop], arecv_l.at[hop])
        await_send(table, asend_s.at[0, hop], arecv_s.at[0, hop])
        await_send(table, asend_s.at[1, hop], arecv_s.at[1, hop])

    give(0, parts - 1)

    def own_rows(ev, out_ref):
        for half in (0, 1):
            for dev in (me, sib):
                pair_unit(ev, 0, away(dev, ev, hops), half)
        if ev == 1:
            ebuf[me] = jnp.broadcast_to(0.5 * jnp.sum(rho[1, 0] + rho[1, 1], keepdims=True), ebuf.shape[1:])

        @pl.loop(0, chunks)
        def _(c):
            out_ref[span(c), :] = force(ev, 0, c)

    own_rows(1, f1_ref)

    @pl.loop(1, n)
    def _(k):
        peer = lax.rem(me + k, n)
        push(ebuf.at[me], esend.at[peer], erecv.at[me], peer)

    own_rows(0, f0_ref)

    for r in range(parts):
        for ev, out_ref in ((1, f1_ref), (0, f0_ref)):
            await_recv(part(pin, ev, r), psend.at[ev, r], precv.at[ev, r])
            for c in range(sub // LANES):
                at = r * (sub // LANES) + c
                out_ref[span(at), :] += pin[ev, span(at), :].astype(F32)

    @pl.loop(1, n)
    def _(p):
        peer = lax.rem(me + p, n)
        await_recv(ebuf.at[peer], esend.at[peer], erecv.at[peer])
        await_send(ebuf.at[me], esend.at[peer], erecv.at[me])

    e_ref[...] = jnp.sum(ebuf[...], axis=0)

    for ev in (0, 1):
        for r in range(parts):
            await_send(part(pout, ev, r), psend.at[ev, r], precv.at[ev, r])


def solution(mesh):
    n = mesh.shape["blk"]
    row_spec = P(("sys", "blk"), None)
    vec_spec = P(("sys", "blk"))

    def local_steps(positions, velocity, charges):
        rows, dim = positions.shape
        hops = n // 4 - 1
        dma = pltpu.SemaphoreType.DMA
        whole = pl.BlockSpec(memory_space=pltpu.VMEM)
        flat = jax.ShapeDtypeStruct((rows, dim), F32)
        force_zero, force_one, energy = pl.pallas_call(
            functools.partial(kernel, n),
            out_shape=(flat, flat, jax.ShapeDtypeStruct((8, LANES), F32)),
            in_specs=[pl.BlockSpec(memory_space=pltpu.HBM)] * 3,
            out_specs=(whole, whole, whole),
            scratch_shapes=[
                pltpu.VMEM((rows, dim), F32),
                pltpu.VMEM((rows, dim), F32),
                pltpu.VMEM((2, n, rows, dim), BF16),
                pltpu.VMEM((n, 3, rows // LANES, LANES), F32),
                pltpu.VMEM((2, 2, rows, LANES), F32),
                pltpu.VMEM((3, rows, LANES), F32),
                pltpu.VMEM((2, 2, rows, dim), F32),
                pltpu.VMEM((2, 2, rows, LANES), F32),
                pltpu.VMEM((2, rows, dim), BF16),
                pltpu.VMEM((2, rows, dim), BF16),
                pltpu.VMEM((n, 8, LANES), F32),
                dma((3,)),
                dma((2, 2 * hops)), dma((2, 2 * hops)), dma((2, 2 * hops)), dma((2, 2 * hops)),
                dma((2, 2 * hops)), dma((2, 2 * hops)), dma((2,)), dma((2,)),
                dma((hops + 1,)), dma((hops + 1,)), dma((hops + 1,)), dma((hops + 1,)),
                dma((2, hops + 1)), dma((2, hops + 1)), dma((2, 4)), dma((2, 4)), dma((n,)), dma((n,)),
            ],
            compiler_params=pltpu.CompilerParams(collective_id=0, has_side_effects=True, vmem_limit_bytes=48 << 20),
            name="leapfrog",
        )(*(pltpu.with_memory_space_constraint(a, pltpu.HBM) for a in
            (positions, velocity, charges.reshape(rows // LANES, LANES))))
        force_zero, force_one = force_zero / dim, force_one / dim
        vel_one = velocity + STEP_SIZE * force_zero
        pos_two = (positions + STEP_SIZE * velocity) + STEP_SIZE * vel_one
        return force_one, energy[0, :1], pos_two, vel_one + STEP_SIZE * force_one

    return jax.shard_map(local_steps, mesh=mesh, in_specs=(row_spec, row_spec, vec_spec),
                         out_specs=(row_spec, P("sys"), row_spec, row_spec), check_vma=False)
```

```python
import functools

import jax
import jax.numpy as jnp
from jax import lax
from jax.experimental import pallas as pl
from jax.experimental.pallas import tpu as pltpu
from jax.sharding import PartitionSpec as P

MESH = pl.DeviceIdType.MESH
STEP_SIZE = 0.5
LOG2E = 1.4426950408889634
LANES = 128
F32 = jnp.float32
BF16 = jnp.bfloat16


def kernel(n, x0_hbm, v0_hbm, q_hbm, f0_ref, f1_ref, e_ref,
           x0_ref, v0_ref, xg, aux, sc, qc, acc, rho, pout, pin, ebuf, in_sem,
           csend, crecv, tsend, trecv, ssend, srecv, own_send, own_recv,
           asend, arecv_r, arecv_l, arecv_s, psend, precv, esend, erecv):
    rows, dim = x0_ref.shape
    unit = rows // 2
    sub = rows // 4
    chunks = rows // LANES
    hops = n // 4 - 1
    scale = 2.0 * LOG2E / (2.0 * dim)
    me = lax.axis_index("blk")
    right = lax.rem(me + 2, n)
    left = lax.rem(me + n - 2, n)
    sib = me + 1 - 2 * lax.rem(me, 2)
    turn = 1 - 2 * lax.rem(me // 2, 2)

    def side(ev):
        return turn * (1 - 2 * ev)

    def away(dev, ev, hop):
        return lax.rem(dev + n - 2 * side(ev) * hop, n)

    def toward(dev, ev, hop):
        return lax.rem(dev + n + 2 * side(ev) * hop, n)

    def push(ref, send, recv, target, dst=None):
        pltpu.make_async_remote_copy(src_ref=ref, dst_ref=ref if dst is None else dst, send_sem=send, recv_sem=recv,
                                     device_id={"blk": target}, device_id_type=MESH).start()

    def await_recv(ref, send, recv):
        pltpu.make_async_remote_copy(src_ref=ref, dst_ref=ref, send_sem=send, recv_sem=recv,
                                     device_id={"blk": sib}, device_id_type=MESH).wait_recv()

    def await_send(ref, send, recv):
        pltpu.make_async_remote_copy(src_ref=ref, dst_ref=ref, send_sem=send, recv_sem=recv,
                                     device_id={"blk": sib}, device_id_type=MESH).wait_send()

    def span(c):
        return pl.ds(pl.multiple_of(c * LANES, LANES), LANES)

    def piece(ev, src, half):
        return xg.at[ev, src, pl.ds(pl.multiple_of(half * unit, unit), unit), :]

    barrier = pltpu.get_barrier_semaphore()
    for peer in (left, right, sib):
        pl.semaphore_signal(barrier, inc=1, device_id={"blk": peer}, device_id_type=MESH)
    front, back = pl.ds(0, unit), pl.ds(unit, unit)
    loads = [pltpu.make_async_copy(src, dst, in_sem.at[k]) for k, (src, dst) in enumerate((
        (v0_hbm.at[front], v0_ref.at[front]), (x0_hbm.at[front], x0_ref.at[front]), (v0_hbm.at[back], v0_ref.at[back]),
        (x0_hbm.at[back], x0_ref.at[back]), (q_hbm, aux.at[me, 0])))]
    for load in loads:
        load.start()

    def round_own(ev, half):
        @pl.loop(half * (chunks // 2), (half + 1) * (chunks // 2))
        def _(c):
            pos = x0_ref[span(c), :]
            xg[ev, me, span(c), :] = (pos + STEP_SIZE * v0_ref[span(c), :] if ev == 1 else pos).astype(BF16)

    loads[0].wait()
    loads[1].wait()
    round_own(1, 0)
    round_own(0, 0)
    loads[2].wait()
    loads[3].wait()
    round_own(1, 1)
    pl.semaphore_wait(barrier, 3)

    def c_push(ev, src, k, half):
        push(piece(ev, src, half), csend.at[0], crecv.at[ev, k], away(me, ev, 1))

    def t_push(ev, src, k, half):
        push(piece(ev, src, half), tsend.at[0], trecv.at[ev, k], toward(me, ev, 1))

    for ev in (1, 0):
        t_push(ev, me, 0, 0)
    round_own(0, 1)
    loads[4].wait()
    for c in range(chunks):
        qc[0, c * LANES:(c + 1) * LANES, :] = jnp.broadcast_to(aux[me, 0, c:c + 1, :], (LANES, LANES)).T
    for ev in (1, 0):
        push(xg.at[ev, me], own_send.at[0], own_recv.at[ev], sib)

    @pl.loop(0, chunks)
    def _(c):
        for ev in (1, 0):
            wide = xg[ev, me, span(c), :].astype(F32)
            norm = jnp.broadcast_to(0.5 * jnp.sum(wide * wide, axis=1, keepdims=True), (LANES, LANES))
            sc[ev, 0, span(c), :] = norm
            aux[me, 1 + ev, pl.ds(c, 1), :] = norm.T[0:1, :]

    acc[...] = jnp.zeros_like(acc)
    rho[...] = jnp.zeros_like(rho)
    push(aux.at[me], asend.at[0], arecv_s.at[0, 0], sib)
    push(aux.at[me], asend.at[0], arecv_r.at[1], right)
    push(aux.at[me], asend.at[0], arecv_l.at[1], left)
    for ev in (1, 0):
        t_push(ev, me, 1, 1)
    for half in (0, 1):
        for ev in (1, 0):
            c_push(ev, me, half, half)

    def pair_rows(ev, party, src, half, start, count, own=False):
        xj = xg[ev, src, pl.ds(pl.multiple_of(half * unit, unit), unit), :]
        base = half * (unit // LANES)
        rs = pl.ds(start, count)
        gram = lax.dot_general(xg[ev, toward(me, ev, party), rs, :], xj, (((1,), (1,)), ((), ())),
                               preferred_element_type=F32)
        norm_i = sc[ev, party, rs, :]
        q_i = qc[party * (1 + ev), rs, :]
        if own:
            diff = lax.broadcasted_iota(jnp.int32, (count, LANES), 0) - lax.broadcasted_iota(jnp.int32, (count, LANES), 1)
        low, total = [], None
        for c in range(unit // LANES):
            norm_j = aux[src, 1 + ev, pl.ds(base + c, 1), :]
            q_j = aux[src, 0, pl.ds(base + c, 1), :]
            neg = jnp.minimum(gram[:, c * LANES:(c + 1) * LANES] - (norm_i + norm_j), 0.0)
            weight = (q_i * q_j) * jnp.exp2(neg * scale)
            if own:
                weight = jnp.where(diff == half * unit + (c * LANES - start), 0.0, weight)
            total = weight if total is None else total + weight
            low.append(weight.astype(BF16))
        rho[ev, party, rs, :] += total
        acc[ev, party, rs, :] += jnp.dot(jnp.concatenate(low, axis=1), xj, preferred_element_type=F32)

    def pair_unit(ev, party, src, half, own=False):
        for r in range(rows // sub):
            pair_rows(ev, party, src, half, r * sub, sub, own)

    await_recv(aux.at[sib], asend.at[0], arecv_s.at[0, 0])
    for ev in (1, 0):
        await_recv(xg.at[ev, sib], own_send.at[0], own_recv.at[ev])

    @pl.loop(0, 2)
    def _(ev):
        for src in (me, sib):
            for half in (0, 1):
                pair_unit(ev, 0, src, half, own=src is me)

    def table_in(hop):
        for k, (step, recv, target) in enumerate(((n - 2 * hop, arecv_r, right), (2 * hop, arecv_l, left))):
            src = lax.rem(me + step, n)
            await_recv(aux.at[src], asend.at[0], recv.at[hop])
            push(aux.at[src], asend.at[0], arecv_s.at[k, hop], sib)
            if hop < hops:
                push(aux.at[src], asend.at[0], recv.at[hop + 1], target)

    def table_sib(hop):
        for k, step in enumerate((n - 2 * hop, 2 * hop)):
            await_recv(aux.at[lax.rem(sib + step, n)], asend.at[0], arecv_s.at[k, hop])

    def c_take(ev, hop, half):
        k = 2 * (hop - 1) + half
        src = away(me, ev, hop)
        await_recv(piece(ev, src, half), csend.at[0], crecv.at[ev, k])
        push(piece(ev, src, half), ssend.at[0], srecv.at[ev, k], sib)

    def c_sib(ev, hop, half):
        k = 2 * (hop - 1) + half
        await_recv(piece(ev, away(sib, ev, hop), half), ssend.at[0], srecv.at[ev, k])

    def t_take(ev, hop, half):
        k = 2 * (hop - 1) + half
        src = toward(me, ev, hop)
        await_recv(piece(ev, src, half), tsend.at[0], trecv.at[ev, k])
        c_push(ev, src, 2 * hop + half, half)

    for half in (0, 1):
        for ev in (1, 0):
            t_take(ev, 1, half)
        if half == 0:
            table_in(1)

    for ev in (1, 0):
        mate = toward(me, ev, 1)

        @pl.loop(0, chunks)
        def _(c):
            sc[ev, 1, span(c), :] = jnp.broadcast_to(aux[mate, 1 + ev, pl.ds(c, 1), :], (LANES, LANES)).T
            qc[1 + ev, span(c), :] = jnp.broadcast_to(aux[mate, 0, pl.ds(c, 1), :], (LANES, LANES)).T

    @pl.loop(0, 2)
    def _(ev):
        for src in (me, sib):
            for half in (0, 1):
                pair_unit(ev, 1, src, half)

    last = 2 * hops - 2

    @pl.loop(0, last)
    def _(k):
        hop = 1 + k // 2
        half = lax.rem(k, 2)
        for ev in (1, 0):
            c_take(ev, hop, half)

            @pl.when(hop == 1)
            def _():
                t_push(ev, away(me, ev, 1), 2 + half, half)

        @pl.when(k == 0)
        def _():
            table_in(2)

        @pl.loop(0, 2)
        def _(ev):
            c_sib(ev, hop, half)

            @pl.when((k == 0) & (ev == 0))
            def _():
                table_sib(1)

            @pl.when((k == 2) & (ev == 0))
            def _():
                table_sib(2)

            for party in (1, 0):
                for dev in (me, sib):
                    pair_unit(ev, party, away(dev, ev, hop), half)

        @pl.when((k == 1) | (k == 2))
        def _():
            for ev in (1, 0):
                t_take(ev, 2, k - 1)

    for ev in (1, 0):
        c_take(ev, hops, 0)
    table_in(3)
    for ev in (1, 0):
        c_sib(ev, hops, 0)
    table_sib(3)

    for ev in (1, 0):
        for dev in (me, sib):
            pair_unit(ev, 1, away(dev, ev, hops), 0)

    def force(ev, party, c):
        held = jnp.sum(rho[ev, party, span(c), :], axis=1, keepdims=True)
        return held * xg[ev, toward(me, ev, party), span(c), :].astype(F32) - acc[ev, party, span(c), :]

    for ev in (1, 0):
        c_take(ev, hops, 1)
    for ev in (1, 0):
        c_sib(ev, hops, 1)

    def part(ref, ev, r):
        return ref.at[ev, pl.ds(pl.multiple_of(r * sub, sub), sub), :]

    def give(ev, r):
        push(part(pout, ev, r), psend.at[0], precv.at[ev, r], toward(me, ev, 1), part(pin, ev, r))

    parts = rows // sub

    @pl.loop(0, 2 * parts)
    def _(j):
        ev = 1 - lax.rem(j, 2)
        r = j // 2
        for dev in (me, sib):
            pair_rows(ev, 1, away(dev, ev, hops), 1, pl.multiple_of(r * sub, sub), sub)

        @pl.when(j > 0)
        def _():
            give(1 - ev, (j - 1) // 2)

        for c in range(sub // LANES):
            at = r * (sub // LANES) + c
            pout[ev, span(at), :] = force(ev, 1, at).astype(BF16)

    await_send(xg.at[0, pl.ds(0, 2 * hops)], csend.at[0], crecv.at[0, 0])
    await_send(xg.at[0, pl.ds(0, 2 * hops)], ssend.at[0], srecv.at[0, 0])
    await_send(xg.at[0, pl.ds(0, 2 * hops - 2)], tsend.at[0], trecv.at[0, 0])
    await_send(xg.at[0, pl.ds(0, 2)], own_send.at[0], own_recv.at[0])
    await_send(aux.at[pl.ds(0, 4 * hops + 1)], asend.at[0], arecv_r.at[0])

    give(0, parts - 1)

    def own_rows(ev, out_ref):
        for half in (0, 1):
            for dev in (me, sib):
                pair_unit(ev, 0, away(dev, ev, hops), half)
        if ev == 1:
            ebuf[me] = jnp.broadcast_to(0.5 * jnp.sum(rho[1, 0] + rho[1, 1], keepdims=True), ebuf.shape[1:])

        @pl.loop(0, chunks)
        def _(c):
            out_ref[span(c), :] = force(ev, 0, c)

    own_rows(1, f1_ref)

    @pl.loop(1, n)
    def _(k):
        peer = lax.rem(me + k, n)
        push(ebuf.at[me], esend.at[0], erecv.at[0], peer)

    own_rows(0, f0_ref)

    for r in range(parts):
        for ev, out_ref in ((1, f1_ref), (0, f0_ref)):
            await_recv(part(pin, ev, r), psend.at[0], precv.at[ev, r])
            for c in range(sub // LANES):
                at = r * (sub // LANES) + c
                out_ref[span(at), :] += pin[ev, span(at), :].astype(F32)

    await_recv(ebuf.at[pl.ds(0, n - 1)], esend.at[0], erecv.at[0])
    e_ref[...] = jnp.sum(ebuf[...], axis=0)
    await_send(ebuf.at[pl.ds(0, n - 1)], esend.at[0], erecv.at[0])
    await_send(pout, psend.at[0], precv.at[0, 0])


def solution(mesh):
    n = mesh.shape["blk"]
    row_spec = P(("sys", "blk"), None)
    vec_spec = P(("sys", "blk"))

    def local_steps(positions, velocity, charges):
        rows, dim = positions.shape
        hops = n // 4 - 1
        dma = pltpu.SemaphoreType.DMA
        whole = pl.BlockSpec(memory_space=pltpu.VMEM)
        flat = jax.ShapeDtypeStruct((rows, dim), F32)
        force_zero, force_one, energy = pl.pallas_call(
            functools.partial(kernel, n),
            out_shape=(flat, flat, jax.ShapeDtypeStruct((8, LANES), F32)),
            in_specs=[pl.BlockSpec(memory_space=pltpu.HBM)] * 3,
            out_specs=(whole, whole, whole),
            scratch_shapes=[
                pltpu.VMEM((rows, dim), F32),
                pltpu.VMEM((rows, dim), F32),
                pltpu.VMEM((2, n, rows, dim), BF16),
                pltpu.VMEM((n, 3, rows // LANES, LANES), F32),
                pltpu.VMEM((2, 2, rows, LANES), F32),
                pltpu.VMEM((3, rows, LANES), F32),
                pltpu.VMEM((2, 2, rows, dim), F32),
                pltpu.VMEM((2, 2, rows, LANES), F32),
                pltpu.VMEM((2, rows, dim), BF16),
                pltpu.VMEM((2, rows, dim), BF16),
                pltpu.VMEM((n, 8, LANES), F32),
                dma((5,)),
                dma((1,)), dma((2, 2 * hops)), dma((1,)), dma((2, 2 * hops - 2)),
                dma((1,)), dma((2, 2 * hops)), dma((1,)), dma((2,)),
                dma((1,)), dma((hops + 1,)), dma((hops + 1,)), dma((2, hops + 1)),
                dma((1,)), dma((2, 4)), dma((1,)), dma((1,)),
            ],
            compiler_params=pltpu.CompilerParams(collective_id=0, has_side_effects=True, vmem_limit_bytes=48 << 20),
            name="leapfrog",
        )(*(pltpu.with_memory_space_constraint(a, pltpu.HBM) for a in
            (positions, velocity, charges.reshape(rows // LANES, LANES))))
        force_zero, force_one = force_zero / dim, force_one / dim
        vel_one = velocity + STEP_SIZE * force_zero
        pos_two = (positions + STEP_SIZE * velocity) + STEP_SIZE * vel_one
        return force_one, energy[0, :1], pos_two, vel_one + STEP_SIZE * force_one

    return jax.shard_map(local_steps, mesh=mesh, in_specs=(row_spec, row_spec, vec_spec),
                         out_specs=(row_spec, P("sys"), row_spec, row_spec), check_vma=False)
```

```python
import functools

import jax
import jax.numpy as jnp
from jax import lax
from jax.experimental import pallas as pl
from jax.experimental.pallas import tpu as pltpu
from jax.sharding import PartitionSpec as P

MESH = pl.DeviceIdType.MESH
STEP_SIZE = 0.5
LOG2E = 1.4426950408889634
LANES = 128
F32 = jnp.float32
BF16 = jnp.bfloat16


def kernel(n, x0_hbm, v0_hbm, q_hbm, f0_ref, f1_ref, e_ref,
           x0_ref, v0_ref, xg, aux, sc, qc, acc, rho, pout, pin, ebuf, in_sem,
           csend, crecv, tsend, trecv, ssend, srecv, own_send, own_recv,
           asend, arecv_r, arecv_l, arecv_s, psend, precv, esend, erecv):
    rows, dim = x0_ref.shape
    unit = rows // 2
    sub = rows // 4
    chunks = rows // LANES
    hops = n // 4 - 1
    scale = 2.0 * LOG2E / (2.0 * dim)
    me = lax.axis_index("blk")
    right = lax.rem(me + 2, n)
    left = lax.rem(me + n - 2, n)
    sib = me + 1 - 2 * lax.rem(me, 2)
    turn = 1 - 2 * lax.rem(me // 2, 2)

    def side(ev):
        return turn * (1 - 2 * ev)

    def away(dev, ev, hop):
        return lax.rem(dev + n - 2 * side(ev) * hop, n)

    def toward(dev, ev, hop):
        return lax.rem(dev + n + 2 * side(ev) * hop, n)

    def push(ref, send, recv, target, dst=None):
        pltpu.make_async_remote_copy(src_ref=ref, dst_ref=ref if dst is None else dst, send_sem=send, recv_sem=recv,
                                     device_id={"blk": target}, device_id_type=MESH).start()

    def await_recv(ref, send, recv):
        pltpu.make_async_remote_copy(src_ref=ref, dst_ref=ref, send_sem=send, recv_sem=recv,
                                     device_id={"blk": sib}, device_id_type=MESH).wait_recv()

    def await_send(ref, send, recv):
        pltpu.make_async_remote_copy(src_ref=ref, dst_ref=ref, send_sem=send, recv_sem=recv,
                                     device_id={"blk": sib}, device_id_type=MESH).wait_send()

    def span(c):
        return pl.ds(pl.multiple_of(c * LANES, LANES), LANES)

    def piece(ev, src, half):
        return xg.at[ev, src, pl.ds(pl.multiple_of(half * unit, unit), unit), :]

    barrier = pltpu.get_barrier_semaphore()
    for peer in (left, right, sib):
        pl.semaphore_signal(barrier, inc=1, device_id={"blk": peer}, device_id_type=MESH)
    front, back = pl.ds(0, unit), pl.ds(unit, unit)
    loads = [pltpu.make_async_copy(src, dst, in_sem.at[k]) for k, (src, dst) in enumerate((
        (v0_hbm.at[front], v0_ref.at[front]), (x0_hbm.at[front], x0_ref.at[front]), (v0_hbm.at[back], v0_ref.at[back]),
        (x0_hbm.at[back], x0_ref.at[back]), (q_hbm, aux.at[me, 0])))]
    for load in loads:
        load.start()

    def round_own(ev, half):
        @pl.loop(half * (chunks // 2), (half + 1) * (chunks // 2))
        def _(c):
            pos = x0_ref[span(c), :]
            xg[ev, me, span(c), :] = (pos + STEP_SIZE * v0_ref[span(c), :] if ev == 1 else pos).astype(BF16)

    loads[0].wait()
    loads[1].wait()
    round_own(1, 0)
    round_own(0, 0)
    loads[2].wait()
    loads[3].wait()
    round_own(1, 1)
    pl.semaphore_wait(barrier, 3)

    def c_push(ev, src, k, half):
        push(piece(ev, src, half), csend.at[0], crecv.at[ev, k], away(me, ev, 1))

    def t_push(ev, src, k, half):
        push(piece(ev, src, half), tsend.at[0], trecv.at[ev, k], toward(me, ev, 1))

    for ev in (1, 0):
        t_push(ev, me, 0, 0)
    round_own(0, 1)
    loads[4].wait()
    for c in range(chunks):
        qc[0, c * LANES:(c + 1) * LANES, :] = jnp.broadcast_to(aux[me, 0, c:c + 1, :], (LANES, LANES)).T
    for ev in (1, 0):
        push(xg.at[ev, me], own_send.at[0], own_recv.at[ev], sib)

    @pl.loop(0, chunks)
    def _(c):
        for ev in (1, 0):
            wide = xg[ev, me, span(c), :].astype(F32)
            norm = jnp.broadcast_to(0.5 * jnp.sum(wide * wide, axis=1, keepdims=True), (LANES, LANES))
            sc[ev, 0, span(c), :] = norm
            aux[me, 1 + ev, pl.ds(c, 1), :] = norm.T[0:1, :]

    acc[...] = jnp.zeros_like(acc)
    rho[...] = jnp.zeros_like(rho)
    push(aux.at[me], asend.at[0], arecv_s.at[0, 0], sib)
    push(aux.at[me], asend.at[0], arecv_r.at[1], right)
    push(aux.at[me], asend.at[0], arecv_l.at[1], left)
    for ev in (1, 0):
        t_push(ev, me, 1, 1)

    def pair_rows(ev, party, src, half, start, count, own=False):
        xj = xg[ev, src, pl.ds(pl.multiple_of(half * unit, unit), unit), :]
        base = half * (unit // LANES)
        rs = pl.ds(start, count)
        gram = lax.dot_general(xg[ev, toward(me, ev, party), rs, :], xj, (((1,), (1,)), ((), ())),
                               preferred_element_type=F32)
        norm_i = sc[ev, party, rs, :]
        q_i = qc[party * (1 + ev), rs, :]
        if own:
            diff = lax.broadcasted_iota(jnp.int32, (count, LANES), 0) - lax.broadcasted_iota(jnp.int32, (count, LANES), 1)
        low, total = [], None
        for c in range(unit // LANES):
            norm_j = aux[src, 1 + ev, pl.ds(base + c, 1), :]
            q_j = aux[src, 0, pl.ds(base + c, 1), :]
            neg = jnp.minimum(gram[:, c * LANES:(c + 1) * LANES] - (norm_i + norm_j), 0.0)
            weight = (q_i * q_j) * jnp.exp2(neg * scale)
            if own:
                weight = jnp.where(diff == half * unit + (c * LANES - start), 0.0, weight)
            total = weight if total is None else total + weight
            low.append(weight.astype(BF16))
        rho[ev, party, rs, :] += total
        acc[ev, party, rs, :] += jnp.dot(jnp.concatenate(low, axis=1), xj, preferred_element_type=F32)

    def pair_unit(ev, party, src, half, own=False):
        for r in range(rows // sub):
            pair_rows(ev, party, src, half, r * sub, sub, own)

    await_recv(aux.at[sib], asend.at[0], arecv_s.at[0, 0])
    for ev in (1, 0):
        await_recv(xg.at[ev, sib], own_send.at[0], own_recv.at[ev])

    @pl.loop(0, 2)
    def _(ev):
        for src in (me, sib):
            for half in (0, 1):
                pair_unit(ev, 0, src, half, own=src is me)

    def table_in(hop):
        for k, (step, recv, target) in enumerate(((n - 2 * hop, arecv_r, right), (2 * hop, arecv_l, left))):
            src = lax.rem(me + step, n)
            await_recv(aux.at[src], asend.at[0], recv.at[hop])
            push(aux.at[src], asend.at[0], arecv_s.at[k, hop], sib)
            if hop < hops:
                push(aux.at[src], asend.at[0], recv.at[hop + 1], target)

    def table_sib(hop):
        for k, step in enumerate((n - 2 * hop, 2 * hop)):
            await_recv(aux.at[lax.rem(sib + step, n)], asend.at[0], arecv_s.at[k, hop])

    def c_take(ev, hop, half):
        k = 2 * (hop - 1) + half
        src = away(me, ev, hop)
        await_recv(piece(ev, src, half), csend.at[0], crecv.at[ev, k])
        push(piece(ev, src, half), ssend.at[0], srecv.at[ev, k], sib)

    def c_sib(ev, hop, half):
        k = 2 * (hop - 1) + half
        await_recv(piece(ev, away(sib, ev, hop), half), ssend.at[0], srecv.at[ev, k])

    def t_wait(ev, hop, half):
        await_recv(piece(ev, toward(me, ev, hop), half), tsend.at[0], trecv.at[ev, 2 * (hop - 1) + half])

    def t_take(ev, hop, half):
        t_wait(ev, hop, half)
        c_push(ev, toward(me, ev, hop), 2 * hop + half, half)

    for ev in (1, 0):
        c_push(ev, me, 0, 0)
    table_in(1)
    for half in (0, 1):
        for ev in (1, 0):
            t_wait(ev, 1, half)
    for ev in (1, 0):
        c_push(ev, me, 1, 1)

    for ev in (1, 0):
        mate = toward(me, ev, 1)

        @pl.loop(0, chunks)
        def _(c):
            sc[ev, 1, span(c), :] = jnp.broadcast_to(aux[mate, 1 + ev, pl.ds(c, 1), :], (LANES, LANES)).T
            qc[1 + ev, span(c), :] = jnp.broadcast_to(aux[mate, 0, pl.ds(c, 1), :], (LANES, LANES)).T

    @pl.loop(0, 2)
    def _(ev):
        for src in (me, sib):
            for half in (0, 1):
                pair_unit(ev, 1, src, half)

    last = 2 * hops - 2

    @pl.loop(0, last)
    def _(k):
        hop = 1 + k // 2
        half = lax.rem(k, 2)
        for ev in (1, 0):
            c_take(ev, hop, half)

            @pl.when(hop == 1)
            def _():
                t_push(ev, away(me, ev, 1), 2 + half, half)
                c_push(ev, toward(me, ev, 1), 2 + half, half)

        @pl.when(k == 0)
        def _():
            table_in(2)

        @pl.loop(0, 2)
        def _(ev):
            c_sib(ev, hop, half)

            @pl.when((k == 0) & (ev == 0))
            def _():
                table_sib(1)

            @pl.when((k == 2) & (ev == 0))
            def _():
                table_sib(2)

            for party in (1, 0):
                for dev in (me, sib):
                    pair_unit(ev, party, away(dev, ev, hop), half)

        @pl.when((k == 1) | (k == 2))
        def _():
            for ev in (1, 0):
                t_take(ev, 2, k - 1)

    for ev in (1, 0):
        c_take(ev, hops, 0)
    table_in(3)
    for ev in (1, 0):
        c_sib(ev, hops, 0)
    table_sib(3)

    for ev in (1, 0):
        for dev in (me, sib):
            pair_unit(ev, 1, away(dev, ev, hops), 0)

    def force(ev, party, c):
        held = jnp.sum(rho[ev, party, span(c), :], axis=1, keepdims=True)
        return held * xg[ev, toward(me, ev, party), span(c), :].astype(F32) - acc[ev, party, span(c), :]

    for ev in (1, 0):
        c_take(ev, hops, 1)
    for ev in (1, 0):
        c_sib(ev, hops, 1)

    def part(ref, ev, r):
        return ref.at[ev, pl.ds(pl.multiple_of(r * sub, sub), sub), :]

    def give(ev, r):
        push(part(pout, ev, r), psend.at[0], precv.at[ev, r], toward(me, ev, 1), part(pin, ev, r))

    parts = rows // sub

    @pl.loop(0, 2 * parts)
    def _(j):
        ev = 1 - lax.rem(j, 2)
        r = j // 2
        for dev in (me, sib):
            pair_rows(ev, 1, away(dev, ev, hops), 1, pl.multiple_of(r * sub, sub), sub)

        @pl.when(j > 0)
        def _():
            give(1 - ev, (j - 1) // 2)

        for c in range(sub // LANES):
            at = r * (sub // LANES) + c
            pout[ev, span(at), :] = force(ev, 1, at).astype(BF16)

    await_send(xg.at[0, pl.ds(0, 2 * hops)], csend.at[0], crecv.at[0, 0])
    await_send(xg.at[0, pl.ds(0, 2 * hops)], ssend.at[0], srecv.at[0, 0])
    await_send(xg.at[0, pl.ds(0, 2 * hops - 2)], tsend.at[0], trecv.at[0, 0])
    await_send(xg.at[0, pl.ds(0, 2)], own_send.at[0], own_recv.at[0])
    await_send(aux.at[pl.ds(0, 4 * hops + 1)], asend.at[0], arecv_r.at[0])

    give(0, parts - 1)

    def own_rows(ev, out_ref):
        for half in (0, 1):
            for dev in (me, sib):
                pair_unit(ev, 0, away(dev, ev, hops), half)
        if ev == 1:
            ebuf[me] = jnp.broadcast_to(0.5 * jnp.sum(rho[1, 0] + rho[1, 1], keepdims=True), ebuf.shape[1:])

        @pl.loop(0, chunks)
        def _(c):
            out_ref[span(c), :] = force(ev, 0, c)

    own_rows(1, f1_ref)

    @pl.loop(1, n)
    def _(k):
        peer = lax.rem(me + k, n)
        push(ebuf.at[me], esend.at[0], erecv.at[0], peer)

    own_rows(0, f0_ref)

    for r in range(parts):
        for ev, out_ref in ((1, f1_ref), (0, f0_ref)):
            await_recv(part(pin, ev, r), psend.at[0], precv.at[ev, r])
            for c in range(sub // LANES):
                at = r * (sub // LANES) + c
                out_ref[span(at), :] += pin[ev, span(at), :].astype(F32)

    await_recv(ebuf.at[pl.ds(0, n - 1)], esend.at[0], erecv.at[0])
    e_ref[...] = jnp.sum(ebuf[...], axis=0)
    await_send(ebuf.at[pl.ds(0, n - 1)], esend.at[0], erecv.at[0])
    await_send(pout, psend.at[0], precv.at[0, 0])


def solution(mesh):
    n = mesh.shape["blk"]
    row_spec = P(("sys", "blk"), None)
    vec_spec = P(("sys", "blk"))

    def local_steps(positions, velocity, charges):
        rows, dim = positions.shape
        hops = n // 4 - 1
        dma = pltpu.SemaphoreType.DMA
        whole = pl.BlockSpec(memory_space=pltpu.VMEM)
        flat = jax.ShapeDtypeStruct((rows, dim), F32)
        force_zero, force_one, energy = pl.pallas_call(
            functools.partial(kernel, n),
            out_shape=(flat, flat, jax.ShapeDtypeStruct((8, LANES), F32)),
            in_specs=[pl.BlockSpec(memory_space=pltpu.HBM)] * 3,
            out_specs=(whole, whole, whole),
            scratch_shapes=[
                pltpu.VMEM((rows, dim), F32),
                pltpu.VMEM((rows, dim), F32),
                pltpu.VMEM((2, n, rows, dim), BF16),
                pltpu.VMEM((n, 3, rows // LANES, LANES), F32),
                pltpu.VMEM((2, 2, rows, LANES), F32),
                pltpu.VMEM((3, rows, LANES), F32),
                pltpu.VMEM((2, 2, rows, dim), F32),
                pltpu.VMEM((2, 2, rows, LANES), F32),
                pltpu.VMEM((2, rows, dim), BF16),
                pltpu.VMEM((2, rows, dim), BF16),
                pltpu.VMEM((n, 8, LANES), F32),
                dma((5,)),
                dma((1,)), dma((2, 2 * hops)), dma((1,)), dma((2, 2 * hops - 2)),
                dma((1,)), dma((2, 2 * hops)), dma((1,)), dma((2,)),
                dma((1,)), dma((hops + 1,)), dma((hops + 1,)), dma((2, hops + 1)),
                dma((1,)), dma((2, 4)), dma((1,)), dma((1,)),
            ],
            compiler_params=pltpu.CompilerParams(collective_id=0, has_side_effects=True, vmem_limit_bytes=48 << 20),
            name="leapfrog",
        )(*(pltpu.with_memory_space_constraint(a, pltpu.HBM) for a in
            (positions, velocity, charges.reshape(rows // LANES, LANES))))
        force_zero, force_one = force_zero / dim, force_one / dim
        vel_one = velocity + STEP_SIZE * force_zero
        pos_two = (positions + STEP_SIZE * velocity) + STEP_SIZE * vel_one
        return force_one, energy[0, :1], pos_two, vel_one + STEP_SIZE * force_one

    return jax.shard_map(local_steps, mesh=mesh, in_specs=(row_spec, row_spec, vec_spec),
                         out_specs=(row_spec, P("sys"), row_spec, row_spec), check_vma=False)
```

```python
import functools

import jax
import jax.numpy as jnp
from jax import lax
from jax.experimental import pallas as pl
from jax.experimental.pallas import tpu as pltpu
from jax.sharding import PartitionSpec as P

MESH = pl.DeviceIdType.MESH
STEP_SIZE = 0.5
LOG2E = 1.4426950408889634
LANES = 128
F32 = jnp.float32
BF16 = jnp.bfloat16


def kernel(n, x0_hbm, v0_hbm, q_hbm, f0_ref, f1_ref, e_ref,
           x0_ref, v0_ref, xg, aux, sc, qc, acc, rho, pout, pin, ebuf, in_sem,
           csend, crecv, tsend, trecv, ssend, srecv, own_send, own_recv,
           asend, arecv_r, arecv_l, arecv_s, psend, precv, esend, erecv):
    rows, dim = x0_ref.shape
    unit = rows // 2
    sub = rows // 4
    chunks = rows // LANES
    hops = n // 4 - 1
    scale = 2.0 * LOG2E / (2.0 * dim)
    me = lax.axis_index("blk")
    right = lax.rem(me + 2, n)
    left = lax.rem(me + n - 2, n)
    sib = me + 1 - 2 * lax.rem(me, 2)
    turn = 1 - 2 * lax.rem(me // 2, 2)

    def side(ev):
        return turn * (1 - 2 * ev)

    def away(dev, ev, hop):
        return lax.rem(dev + n - 2 * side(ev) * hop, n)

    def toward(dev, ev, hop):
        return lax.rem(dev + n + 2 * side(ev) * hop, n)

    def push(ref, send, recv, target, dst=None):
        pltpu.make_async_remote_copy(src_ref=ref, dst_ref=ref if dst is None else dst, send_sem=send, recv_sem=recv,
                                     device_id={"blk": target}, device_id_type=MESH).start()

    def await_recv(ref, send, recv):
        pltpu.make_async_remote_copy(src_ref=ref, dst_ref=ref, send_sem=send, recv_sem=recv,
                                     device_id={"blk": sib}, device_id_type=MESH).wait_recv()

    def await_send(ref, send, recv):
        pltpu.make_async_remote_copy(src_ref=ref, dst_ref=ref, send_sem=send, recv_sem=recv,
                                     device_id={"blk": sib}, device_id_type=MESH).wait_send()

    def span(c):
        return pl.ds(pl.multiple_of(c * LANES, LANES), LANES)

    def piece(ev, src, half):
        return xg.at[ev, src, pl.ds(pl.multiple_of(half * unit, unit), unit), :]

    barrier = pltpu.get_barrier_semaphore()
    for peer in (left, right, sib):
        pl.semaphore_signal(barrier, inc=1, device_id={"blk": peer}, device_id_type=MESH)
    front, back = pl.ds(0, unit), pl.ds(unit, unit)
    loads = [pltpu.make_async_copy(src, dst, in_sem.at[k]) for k, (src, dst) in enumerate((
        (v0_hbm.at[front], v0_ref.at[front]), (x0_hbm.at[front], x0_ref.at[front]), (v0_hbm.at[back], v0_ref.at[back]),
        (x0_hbm.at[back], x0_ref.at[back]), (q_hbm, aux.at[me, 0])))]
    for load in loads:
        load.start()

    def round_own(ev, half):
        @pl.loop(half * (chunks // 2), (half + 1) * (chunks // 2))
        def _(c):
            pos = x0_ref[span(c), :]
            xg[ev, me, span(c), :] = (pos + STEP_SIZE * v0_ref[span(c), :] if ev == 1 else pos).astype(BF16)

    loads[0].wait()
    loads[1].wait()
    round_own(1, 0)
    round_own(0, 0)
    loads[2].wait()
    loads[3].wait()
    round_own(1, 1)
    pl.semaphore_wait(barrier, 3)

    def c_push(ev, src, k, half):
        push(piece(ev, src, half), csend.at[0], crecv.at[ev, k], away(me, ev, 1))

    def t_push(ev, src, k, half):
        push(piece(ev, src, half), tsend.at[0], trecv.at[ev, k], toward(me, ev, 1))

    for ev in (1, 0):
        t_push(ev, me, 0, 0)
    round_own(0, 1)
    loads[4].wait()
    for c in range(chunks):
        qc[0, c * LANES:(c + 1) * LANES, :] = jnp.broadcast_to(aux[me, 0, c:c + 1, :], (LANES, LANES)).T
    for ev in (1, 0):
        push(xg.at[ev, me], own_send.at[0], own_recv.at[ev], sib)

    @pl.loop(0, chunks)
    def _(c):
        for ev in (1, 0):
            wide = xg[ev, me, span(c), :].astype(F32)
            norm = jnp.broadcast_to(0.5 * jnp.sum(wide * wide, axis=1, keepdims=True), (LANES, LANES))
            sc[ev, 0, span(c), :] = norm
            aux[me, 1 + ev, pl.ds(c, 1), :] = norm.T[0:1, :]

    acc[...] = jnp.zeros_like(acc)
    rho[...] = jnp.zeros_like(rho)
    push(aux.at[me], asend.at[0], arecv_s.at[0, 0], sib)
    push(aux.at[me], asend.at[0], arecv_r.at[1], right)
    push(aux.at[me], asend.at[0], arecv_l.at[1], left)
    for ev in (1, 0):
        t_push(ev, me, 1, 1)

    def pair_rows(ev, party, src, half, start, count, own=False):
        xj = xg[ev, src, pl.ds(pl.multiple_of(half * unit, unit), unit), :]
        base = half * (unit // LANES)
        rs = pl.ds(start, count)
        gram = lax.dot_general(xg[ev, toward(me, ev, party), rs, :], xj, (((1,), (1,)), ((), ())),
                               preferred_element_type=F32)
        norm_i = sc[ev, party, rs, :]
        q_i = qc[party * (1 + ev), rs, :]
        if own:
            diff = lax.broadcasted_iota(jnp.int32, (count, LANES), 0) - lax.broadcasted_iota(jnp.int32, (count, LANES), 1)
        low, total = [], None
        for c in range(unit // LANES):
            norm_j = aux[src, 1 + ev, pl.ds(base + c, 1), :]
            q_j = aux[src, 0, pl.ds(base + c, 1), :]
            neg = jnp.minimum(gram[:, c * LANES:(c + 1) * LANES] - (norm_i + norm_j), 0.0)
            weight = (q_i * q_j) * jnp.exp2(neg * scale)
            if own:
                weight = jnp.where(diff == half * unit + (c * LANES - start), 0.0, weight)
            total = weight if total is None else total + weight
            low.append(weight.astype(BF16))
        rho[ev, party, rs, :] += total
        acc[ev, party, rs, :] += jnp.dot(jnp.concatenate(low, axis=1), xj, preferred_element_type=F32)

    def pair_unit(ev, party, src, half, own=False):
        for r in range(rows // sub):
            pair_rows(ev, party, src, half, r * sub, sub, own)

    await_recv(aux.at[sib], asend.at[0], arecv_s.at[0, 0])
    for ev in (1, 0):
        await_recv(xg.at[ev, sib], own_send.at[0], own_recv.at[ev])

    @pl.loop(0, 2)
    def _(ev):
        for src in (me, sib):
            for half in (0, 1):
                pair_unit(ev, 0, src, half, own=src is me)

    def table_in(hop):
        for k, (step, recv, target) in enumerate(((n - 2 * hop, arecv_r, right), (2 * hop, arecv_l, left))):
            src = lax.rem(me + step, n)
            await_recv(aux.at[src], asend.at[0], recv.at[hop])
            push(aux.at[src], asend.at[0], arecv_s.at[k, hop], sib)
            if hop < hops:
                push(aux.at[src], asend.at[0], recv.at[hop + 1], target)

    def table_sib(hop):
        for k, step in enumerate((n - 2 * hop, 2 * hop)):
            await_recv(aux.at[lax.rem(sib + step, n)], asend.at[0], arecv_s.at[k, hop])

    def c_take(ev, hop, half):
        k = 2 * (hop - 1) + half
        src = away(me, ev, hop)
        await_recv(piece(ev, src, half), csend.at[0], crecv.at[ev, k])
        push(piece(ev, src, half), ssend.at[0], srecv.at[ev, k], sib)

    def c_sib(ev, hop, half):
        k = 2 * (hop - 1) + half
        await_recv(piece(ev, away(sib, ev, hop), half), ssend.at[0], srecv.at[ev, k])

    def t_wait(ev, hop, half):
        await_recv(piece(ev, toward(me, ev, hop), half), tsend.at[0], trecv.at[ev, 2 * (hop - 1) + half])

    def t_take(ev, hop, half):
        t_wait(ev, hop, half)
        c_push(ev, toward(me, ev, hop), 2 * hop + half, half)

    for ev in (1, 0):
        c_push(ev, me, 0, 0)
    table_in(1)
    for half in (0, 1):
        for ev in (1, 0):
            t_wait(ev, 1, half)
    for ev in (1, 0):
        c_push(ev, me, 1, 1)

    for ev in (1, 0):
        mate = toward(me, ev, 1)

        @pl.loop(0, chunks)
        def _(c):
            sc[ev, 1, span(c), :] = jnp.broadcast_to(aux[mate, 1 + ev, pl.ds(c, 1), :], (LANES, LANES)).T
            qc[1 + ev, span(c), :] = jnp.broadcast_to(aux[mate, 0, pl.ds(c, 1), :], (LANES, LANES)).T

    @pl.loop(0, 2)
    def _(ev):
        for src in (me, sib):
            for half in (0, 1):
                pair_unit(ev, 1, src, half)

    last = 2 * hops - 2

    @pl.loop(0, last)
    def _(k):
        hop = 1 + k // 2
        half = lax.rem(k, 2)
        for ev in (1, 0):
            c_take(ev, hop, half)

            @pl.when(hop == 1)
            def _():
                t_push(ev, away(me, ev, 1), 2 + half, half)

        @pl.when(hop > 1)
        def _():
            for ev in (1, 0):
                t_take(ev, 2, half)

        @pl.when(k == 0)
        def _():
            table_in(2)

        @pl.loop(0, 2)
        def _(ev):
            c_sib(ev, hop, half)

            @pl.when((k == 0) & (ev == 0))
            def _():
                table_sib(1)

            @pl.when((k == 2) & (ev == 0))
            def _():
                table_sib(2)

            for party in (1, 0):
                for dev in (me, sib):
                    pair_unit(ev, party, away(dev, ev, hop), half)

        @pl.when(hop == 1)
        def _():
            for ev in (1, 0):
                c_push(ev, toward(me, ev, 1), 2 + half, half)

    for ev in (1, 0):
        c_take(ev, hops, 0)
    table_in(3)
    for ev in (1, 0):
        c_sib(ev, hops, 0)
    table_sib(3)

    for ev in (1, 0):
        for dev in (me, sib):
            pair_unit(ev, 1, away(dev, ev, hops), 0)

    def force(ev, party, c):
        held = jnp.sum(rho[ev, party, span(c), :], axis=1, keepdims=True)
        return held * xg[ev, toward(me, ev, party), span(c), :].astype(F32) - acc[ev, party, span(c), :]

    for ev in (1, 0):
        c_take(ev, hops, 1)
    for ev in (1, 0):
        c_sib(ev, hops, 1)

    def part(ref, ev, r):
        return ref.at[ev, pl.ds(pl.multiple_of(r * sub, sub), sub), :]

    def give(ev, r):
        push(part(pout, ev, r), psend.at[0], precv.at[ev, r], toward(me, ev, 1), part(pin, ev, r))

    parts = rows // sub

    @pl.loop(0, 2 * parts)
    def _(j):
        ev = 1 - lax.rem(j, 2)
        r = j // 2
        for dev in (me, sib):
            pair_rows(ev, 1, away(dev, ev, hops), 1, pl.multiple_of(r * sub, sub), sub)

        @pl.when(j > 0)
        def _():
            give(1 - ev, (j - 1) // 2)

        for c in range(sub // LANES):
            at = r * (sub // LANES) + c
            pout[ev, span(at), :] = force(ev, 1, at).astype(BF16)

    await_send(xg.at[0, pl.ds(0, 2 * hops)], csend.at[0], crecv.at[0, 0])
    await_send(xg.at[0, pl.ds(0, 2 * hops)], ssend.at[0], srecv.at[0, 0])
    await_send(xg.at[0, pl.ds(0, 2 * hops - 2)], tsend.at[0], trecv.at[0, 0])
    await_send(xg.at[0, pl.ds(0, 2)], own_send.at[0], own_recv.at[0])
    await_send(aux.at[pl.ds(0, 4 * hops + 1)], asend.at[0], arecv_r.at[0])

    give(0, parts - 1)

    def own_rows(ev, out_ref):
        for half in (0, 1):
            for dev in (me, sib):
                pair_unit(ev, 0, away(dev, ev, hops), half)
        if ev == 1:
            ebuf[me] = jnp.broadcast_to(0.5 * jnp.sum(rho[1, 0] + rho[1, 1], keepdims=True), ebuf.shape[1:])

        @pl.loop(0, chunks)
        def _(c):
            out_ref[span(c), :] = force(ev, 0, c)

    own_rows(1, f1_ref)

    @pl.loop(1, n)
    def _(k):
        peer = lax.rem(me + k, n)
        push(ebuf.at[me], esend.at[0], erecv.at[0], peer)

    own_rows(0, f0_ref)

    for r in range(parts):
        for ev, out_ref in ((1, f1_ref), (0, f0_ref)):
            await_recv(part(pin, ev, r), psend.at[0], precv.at[ev, r])
            for c in range(sub // LANES):
                at = r * (sub // LANES) + c
                out_ref[span(at), :] += pin[ev, span(at), :].astype(F32)

    await_recv(ebuf.at[pl.ds(0, n - 1)], esend.at[0], erecv.at[0])
    e_ref[...] = jnp.sum(ebuf[...], axis=0)
    await_send(ebuf.at[pl.ds(0, n - 1)], esend.at[0], erecv.at[0])
    await_send(pout, psend.at[0], precv.at[0, 0])


def solution(mesh):
    n = mesh.shape["blk"]
    row_spec = P(("sys", "blk"), None)
    vec_spec = P(("sys", "blk"))

    def local_steps(positions, velocity, charges):
        rows, dim = positions.shape
        hops = n // 4 - 1
        dma = pltpu.SemaphoreType.DMA
        whole = pl.BlockSpec(memory_space=pltpu.VMEM)
        flat = jax.ShapeDtypeStruct((rows, dim), F32)
        force_zero, force_one, energy = pl.pallas_call(
            functools.partial(kernel, n),
            out_shape=(flat, flat, jax.ShapeDtypeStruct((8, LANES), F32)),
            in_specs=[pl.BlockSpec(memory_space=pltpu.HBM)] * 3,
            out_specs=(whole, whole, whole),
            scratch_shapes=[
                pltpu.VMEM((rows, dim), F32),
                pltpu.VMEM((rows, dim), F32),
                pltpu.VMEM((2, n, rows, dim), BF16),
                pltpu.VMEM((n, 3, rows // LANES, LANES), F32),
                pltpu.VMEM((2, 2, rows, LANES), F32),
                pltpu.VMEM((3, rows, LANES), F32),
                pltpu.VMEM((2, 2, rows, dim), F32),
                pltpu.VMEM((2, 2, rows, LANES), F32),
                pltpu.VMEM((2, rows, dim), BF16),
                pltpu.VMEM((2, rows, dim), BF16),
                pltpu.VMEM((n, 8, LANES), F32),
                dma((5,)),
                dma((1,)), dma((2, 2 * hops)), dma((1,)), dma((2, 2 * hops - 2)),
                dma((1,)), dma((2, 2 * hops)), dma((1,)), dma((2,)),
                dma((1,)), dma((hops + 1,)), dma((hops + 1,)), dma((2, hops + 1)),
                dma((1,)), dma((2, 4)), dma((1,)), dma((1,)),
            ],
            compiler_params=pltpu.CompilerParams(collective_id=0, has_side_effects=True, vmem_limit_bytes=48 << 20),
            name="leapfrog",
        )(*(pltpu.with_memory_space_constraint(a, pltpu.HBM) for a in
            (positions, velocity, charges.reshape(rows // LANES, LANES))))
        force_zero, force_one = force_zero / dim, force_one / dim
        vel_one = velocity + STEP_SIZE * force_zero
        pos_two = (positions + STEP_SIZE * velocity) + STEP_SIZE * vel_one
        return force_one, energy[0, :1], pos_two, vel_one + STEP_SIZE * force_one

    return jax.shard_map(local_steps, mesh=mesh, in_specs=(row_spec, row_spec, vec_spec),
                         out_specs=(row_spec, P("sys"), row_spec, row_spec), check_vma=False)
```

```python
import functools

import jax
import jax.numpy as jnp
from jax import lax
from jax.experimental import pallas as pl
from jax.experimental.pallas import tpu as pltpu
from jax.sharding import PartitionSpec as P

MESH = pl.DeviceIdType.MESH
STEP_SIZE = 0.5
LOG2E = 1.4426950408889634
LANES = 128
F32 = jnp.float32
BF16 = jnp.bfloat16


def kernel(n, x0_hbm, v0_hbm, q_hbm, f0_ref, f1_ref, e_ref,
           x0_ref, v0_ref, xg, aux, sc, qc, acc, rho, pout, pin, ebuf, in_sem,
           csend, crecv, tsend, trecv, ssend, srecv, own_send, own_recv,
           asend, arecv_r, arecv_l, arecv_s, psend, precv, esend, erecv):
    rows, dim = x0_ref.shape
    unit = rows // 2
    sub = rows // 4
    chunks = rows // LANES
    hops = n // 4 - 1
    scale = 2.0 * LOG2E / (2.0 * dim)
    me = lax.axis_index("blk")
    right = lax.rem(me + 2, n)
    left = lax.rem(me + n - 2, n)
    sib = me + 1 - 2 * lax.rem(me, 2)
    turn = 1 - 2 * lax.rem(me // 2, 2)

    def side(ev):
        return turn * (1 - 2 * ev)

    def away(dev, ev, hop):
        return lax.rem(dev + n - 2 * side(ev) * hop, n)

    def toward(dev, ev, hop):
        return lax.rem(dev + n + 2 * side(ev) * hop, n)

    def push(ref, send, recv, target, dst=None):
        pltpu.make_async_remote_copy(src_ref=ref, dst_ref=ref if dst is None else dst, send_sem=send, recv_sem=recv,
                                     device_id={"blk": target}, device_id_type=MESH).start()

    def await_recv(ref, send, recv):
        pltpu.make_async_remote_copy(src_ref=ref, dst_ref=ref, send_sem=send, recv_sem=recv,
                                     device_id={"blk": sib}, device_id_type=MESH).wait_recv()

    def await_send(ref, send, recv):
        pltpu.make_async_remote_copy(src_ref=ref, dst_ref=ref, send_sem=send, recv_sem=recv,
                                     device_id={"blk": sib}, device_id_type=MESH).wait_send()

    def span(c):
        return pl.ds(pl.multiple_of(c * LANES, LANES), LANES)

    def piece(ev, src, half):
        return xg.at[ev, src, pl.ds(pl.multiple_of(half * unit, unit), unit), :]

    barrier = pltpu.get_barrier_semaphore()
    for peer in (left, right, sib):
        pl.semaphore_signal(barrier, inc=1, device_id={"blk": peer}, device_id_type=MESH)
    front, back = pl.ds(0, unit), pl.ds(unit, unit)
    loads = [pltpu.make_async_copy(src, dst, in_sem.at[k]) for k, (src, dst) in enumerate((
        (v0_hbm.at[front], v0_ref.at[front]), (x0_hbm.at[front], x0_ref.at[front]), (v0_hbm.at[back], v0_ref.at[back]),
        (x0_hbm.at[back], x0_ref.at[back]), (q_hbm, aux.at[me, 0])))]
    for load in loads:
        load.start()

    def round_own(ev, half):
        @pl.loop(half * (chunks // 2), (half + 1) * (chunks // 2))
        def _(c):
            pos = x0_ref[span(c), :]
            xg[ev, me, span(c), :] = (pos + STEP_SIZE * v0_ref[span(c), :] if ev == 1 else pos).astype(BF16)

    loads[0].wait()
    loads[1].wait()
    round_own(1, 0)
    round_own(0, 0)
    loads[2].wait()
    loads[3].wait()
    round_own(1, 1)
    pl.semaphore_wait(barrier, 3)

    def c_push(ev, src, k, half):
        push(piece(ev, src, half), csend.at[0], crecv.at[ev, k], away(me, ev, 1))

    def t_push(ev, src, k, half):
        push(piece(ev, src, half), tsend.at[0], trecv.at[ev, k], toward(me, ev, 1))

    for ev in (1, 0):
        t_push(ev, me, 0, 0)
    round_own(0, 1)
    loads[4].wait()
    for c in range(chunks):
        qc[0, c * LANES:(c + 1) * LANES, :] = jnp.broadcast_to(aux[me, 0, c:c + 1, :], (LANES, LANES)).T
    for ev in (1, 0):
        push(xg.at[ev, me], own_send.at[0], own_recv.at[ev], sib)

    @pl.loop(0, chunks)
    def _(c):
        for ev in (1, 0):
            wide = xg[ev, me, span(c), :].astype(F32)
            norm = jnp.broadcast_to(0.5 * jnp.sum(wide * wide, axis=1, keepdims=True), (LANES, LANES))
            sc[ev, 0, span(c), :] = norm
            aux[me, 1 + ev, pl.ds(c, 1), :] = norm.T[0:1, :]

    acc[...] = jnp.zeros_like(acc)
    rho[...] = jnp.zeros_like(rho)
    push(aux.at[me], asend.at[0], arecv_s.at[0, 0], sib)
    push(aux.at[me], asend.at[0], arecv_r.at[1], right)
    push(aux.at[me], asend.at[0], arecv_l.at[1], left)
    for ev in (1, 0):
        t_push(ev, me, 1, 1)

    def pair_rows(ev, party, src, half, start, count, own=False):
        xj = xg[ev, src, pl.ds(pl.multiple_of(half * unit, unit), unit), :]
        base = half * (unit // LANES)
        rs = pl.ds(start, count)
        gram = lax.dot_general(xg[ev, toward(me, ev, party), rs, :], xj, (((1,), (1,)), ((), ())),
                               preferred_element_type=F32)
        norm_i = sc[ev, party, rs, :]
        q_i = qc[party * (1 + ev), rs, :]
        if own:
            diff = lax.broadcasted_iota(jnp.int32, (count, LANES), 0) - lax.broadcasted_iota(jnp.int32, (count, LANES), 1)
        low, total = [], None
        for c in range(unit // LANES):
            norm_j = aux[src, 1 + ev, pl.ds(base + c, 1), :]
            q_j = aux[src, 0, pl.ds(base + c, 1), :]
            neg = jnp.minimum(gram[:, c * LANES:(c + 1) * LANES] - (norm_i + norm_j), 0.0)
            weight = (q_i * q_j) * jnp.exp2(neg * scale)
            if own:
                weight = jnp.where(diff == half * unit + (c * LANES - start), 0.0, weight)
            total = weight if total is None else total + weight
            low.append(weight.astype(BF16))
        rho[ev, party, rs, :] += total
        acc[ev, party, rs, :] += jnp.dot(jnp.concatenate(low, axis=1), xj, preferred_element_type=F32)

    def pair_unit(ev, party, src, half, own=False):
        for r in range(rows // sub):
            pair_rows(ev, party, src, half, r * sub, sub, own)

    await_recv(aux.at[sib], asend.at[0], arecv_s.at[0, 0])
    for ev in (1, 0):
        await_recv(xg.at[ev, sib], own_send.at[0], own_recv.at[ev])

    @pl.loop(0, 2)
    def _(ev):
        for src in (me, sib):
            for half in (0, 1):
                pair_unit(ev, 0, src, half, own=src is me)

    def table_in(hop):
        for k, (step, recv, target) in enumerate(((n - 2 * hop, arecv_r, right), (2 * hop, arecv_l, left))):
            src = lax.rem(me + step, n)
            await_recv(aux.at[src], asend.at[0], recv.at[hop])
            push(aux.at[src], asend.at[0], arecv_s.at[k, hop], sib)
            if hop < hops:
                push(aux.at[src], asend.at[0], recv.at[hop + 1], target)

    def table_sib(hop):
        for k, step in enumerate((n - 2 * hop, 2 * hop)):
            await_recv(aux.at[lax.rem(sib + step, n)], asend.at[0], arecv_s.at[k, hop])

    def c_take(ev, hop, half):
        k = 2 * (hop - 1) + half
        src = away(me, ev, hop)
        await_recv(piece(ev, src, half), csend.at[0], crecv.at[ev, k])
        push(piece(ev, src, half), ssend.at[0], srecv.at[ev, k], sib)

    def c_sib(ev, hop, half):
        k = 2 * (hop - 1) + half
        await_recv(piece(ev, away(sib, ev, hop), half), ssend.at[0], srecv.at[ev, k])

    def t_wait(ev, hop, half):
        await_recv(piece(ev, toward(me, ev, hop), half), tsend.at[0], trecv.at[ev, 2 * (hop - 1) + half])

    def t_take(ev, hop, half):
        t_wait(ev, hop, half)
        c_push(ev, toward(me, ev, hop), 2 * hop + half, half)

    for ev in (1, 0):
        c_push(ev, me, 0, 0)
    table_in(1)
    for half in (0, 1):
        for ev in (1, 0):
            t_wait(ev, 1, half)
    for ev in (1, 0):
        c_push(ev, me, 1, 1)

    for ev in (1, 0):
        mate = toward(me, ev, 1)

        @pl.loop(0, chunks)
        def _(c):
            sc[ev, 1, span(c), :] = jnp.broadcast_to(aux[mate, 1 + ev, pl.ds(c, 1), :], (LANES, LANES)).T
            qc[1 + ev, span(c), :] = jnp.broadcast_to(aux[mate, 0, pl.ds(c, 1), :], (LANES, LANES)).T

    @pl.loop(0, 2)
    def _(ev):
        for src in (me, sib):
            for half in (0, 1):
                pair_unit(ev, 1, src, half)

    last = 2 * hops - 2

    @pl.loop(0, last)
    def _(k):
        hop = 1 + k // 2
        half = lax.rem(k, 2)
        for ev in (1, 0):
            c_take(ev, hop, half)

            @pl.when(hop == 1)
            def _():
                t_push(ev, away(me, ev, 1), 2 + half, half)
                c_push(ev, toward(me, ev, 1), 2 + half, half)

        @pl.when(hop > 1)
        def _():
            for ev in (1, 0):
                t_take(ev, 2, half)

        @pl.when(k == 0)
        def _():
            table_in(2)

        @pl.loop(0, 2)
        def _(ev):
            c_sib(ev, hop, half)

            @pl.when((k == 0) & (ev == 0))
            def _():
                table_sib(1)

            @pl.when((k == 2) & (ev == 0))
            def _():
                table_sib(2)

            for party in (1, 0):
                for dev in (me, sib):
                    pair_unit(ev, party, away(dev, ev, hop), half)

    for ev in (1, 0):
        c_take(ev, hops, 0)
    table_in(3)
    for ev in (1, 0):
        c_sib(ev, hops, 0)
    table_sib(3)

    for ev in (1, 0):
        for dev in (me, sib):
            pair_unit(ev, 1, away(dev, ev, hops), 0)

    def force(ev, party, c):
        held = jnp.sum(rho[ev, party, span(c), :], axis=1, keepdims=True)
        return held * xg[ev, toward(me, ev, party), span(c), :].astype(F32) - acc[ev, party, span(c), :]

    for ev in (1, 0):
        c_take(ev, hops, 1)
    for ev in (1, 0):
        c_sib(ev, hops, 1)

    def part(ref, ev, r):
        return ref.at[ev, pl.ds(pl.multiple_of(r * sub, sub), sub), :]

    def give(ev, r):
        push(part(pout, ev, r), psend.at[0], precv.at[ev, r], toward(me, ev, 1), part(pin, ev, r))

    parts = rows // sub

    @pl.loop(0, 2 * parts)
    def _(j):
        ev = 1 - lax.rem(j, 2)
        r = j // 2
        for dev in (me, sib):
            pair_rows(ev, 1, away(dev, ev, hops), 1, pl.multiple_of(r * sub, sub), sub)

        @pl.when(j > 0)
        def _():
            give(1 - ev, (j - 1) // 2)

        for c in range(sub // LANES):
            at = r * (sub // LANES) + c
            pout[ev, span(at), :] = force(ev, 1, at).astype(BF16)

    await_send(xg.at[0, pl.ds(0, 2 * hops)], csend.at[0], crecv.at[0, 0])
    await_send(xg.at[0, pl.ds(0, 2 * hops)], ssend.at[0], srecv.at[0, 0])
    await_send(xg.at[0, pl.ds(0, 2 * hops - 2)], tsend.at[0], trecv.at[0, 0])
    await_send(xg.at[0, pl.ds(0, 2)], own_send.at[0], own_recv.at[0])
    await_send(aux.at[pl.ds(0, 4 * hops + 1)], asend.at[0], arecv_r.at[0])

    give(0, parts - 1)

    def own_rows(ev, out_ref):
        for half in (0, 1):
            for dev in (me, sib):
                pair_unit(ev, 0, away(dev, ev, hops), half)
        if ev == 1:
            ebuf[me] = jnp.broadcast_to(0.5 * jnp.sum(rho[1, 0] + rho[1, 1], keepdims=True), ebuf.shape[1:])

        @pl.loop(0, chunks)
        def _(c):
            out_ref[span(c), :] = force(ev, 0, c)

    own_rows(1, f1_ref)

    @pl.loop(1, n)
    def _(k):
        peer = lax.rem(me + k, n)
        push(ebuf.at[me], esend.at[0], erecv.at[0], peer)

    own_rows(0, f0_ref)

    for r in range(parts):
        for ev, out_ref in ((1, f1_ref), (0, f0_ref)):
            await_recv(part(pin, ev, r), psend.at[0], precv.at[ev, r])
            for c in range(sub // LANES):
                at = r * (sub // LANES) + c
                out_ref[span(at), :] += pin[ev, span(at), :].astype(F32)

    await_recv(ebuf.at[pl.ds(0, n - 1)], esend.at[0], erecv.at[0])
    e_ref[...] = jnp.sum(ebuf[...], axis=0)
    await_send(ebuf.at[pl.ds(0, n - 1)], esend.at[0], erecv.at[0])
    await_send(pout, psend.at[0], precv.at[0, 0])


def solution(mesh):
    n = mesh.shape["blk"]
    row_spec = P(("sys", "blk"), None)
    vec_spec = P(("sys", "blk"))

    def local_steps(positions, velocity, charges):
        rows, dim = positions.shape
        hops = n // 4 - 1
        dma = pltpu.SemaphoreType.DMA
        whole = pl.BlockSpec(memory_space=pltpu.VMEM)
        flat = jax.ShapeDtypeStruct((rows, dim), F32)
        force_zero, force_one, energy = pl.pallas_call(
            functools.partial(kernel, n),
            out_shape=(flat, flat, jax.ShapeDtypeStruct((8, LANES), F32)),
            in_specs=[pl.BlockSpec(memory_space=pltpu.HBM)] * 3,
            out_specs=(whole, whole, whole),
            scratch_shapes=[
                pltpu.VMEM((rows, dim), F32),
                pltpu.VMEM((rows, dim), F32),
                pltpu.VMEM((2, n, rows, dim), BF16),
                pltpu.VMEM((n, 3, rows // LANES, LANES), F32),
                pltpu.VMEM((2, 2, rows, LANES), F32),
                pltpu.VMEM((3, rows, LANES), F32),
                pltpu.VMEM((2, 2, rows, dim), F32),
                pltpu.VMEM((2, 2, rows, LANES), F32),
                pltpu.VMEM((2, rows, dim), BF16),
                pltpu.VMEM((2, rows, dim), BF16),
                pltpu.VMEM((n, 8, LANES), F32),
                dma((5,)),
                dma((1,)), dma((2, 2 * hops)), dma((1,)), dma((2, 2 * hops - 2)),
                dma((1,)), dma((2, 2 * hops)), dma((1,)), dma((2,)),
                dma((1,)), dma((hops + 1,)), dma((hops + 1,)), dma((2, hops + 1)),
                dma((1,)), dma((2, 4)), dma((1,)), dma((1,)),
            ],
            compiler_params=pltpu.CompilerParams(collective_id=0, has_side_effects=True, vmem_limit_bytes=48 << 20),
            name="leapfrog",
        )(*(pltpu.with_memory_space_constraint(a, pltpu.HBM) for a in
            (positions, velocity, charges.reshape(rows // LANES, LANES))))
        force_zero, force_one = force_zero / dim, force_one / dim
        vel_one = velocity + STEP_SIZE * force_zero
        pos_two = (positions + STEP_SIZE * velocity) + STEP_SIZE * vel_one
        return force_one, energy[0, :1], pos_two, vel_one + STEP_SIZE * force_one

    return jax.shard_map(local_steps, mesh=mesh, in_specs=(row_spec, row_spec, vec_spec),
                         out_specs=(row_spec, P("sys"), row_spec, row_spec), check_vma=False)
```
